768 devices in a mesh: pipe: 12 (over z), dp: 16 (over x, y_hi), tensor: 4 (over y_lo, core).
Axes of the slice: x: 4, y: 8 (y_hi: 4, y_lo: 2; y = y_hi * 2 + y_lo), z: 12, core: 2. Of those that a mesh axis runs over, the one named last changes fastest.
Arguments:
- saved_inputs: bfloat16 [3, 2, 12, 2048, 4096], P(None, None, 'pipe', 'dp', 'tensor'), may hold values from -6 to 6
- proj_in: bfloat16 [2, 12, 512, 4096], P(None, 'pipe', None, 'tensor'), may hold values from -0.09375 to 0.09375
- proj_out: bfloat16 [2, 12, 512, 4096], P(None, 'pipe', None, 'tensor'), may hold values from -0.25 to 0.25
- norm_gain: float32 [2, 12, 4096], P(None, 'pipe', 'tensor'), may hold values from 0.1 to 1.9
- arriving: bfloat16 [2, 12, 2048, 4096], P(None, 'pipe', 'dp', 'tensor'), may hold values from -6 to 6
- logp_grad: bfloat16 [2, 2048, 4096], P(None, 'dp', 'tensor'), may hold values from -6 to 6
- rewards: float32 [2, 16, 4], P(None, 'dp'), may hold values from -4 to 4
- seq_lengths: int32 [2, 16, 4], P(None, 'dp'), may hold values from 1 to 64, 128 in all within a row
- group_ids: int32 [2, 16, 4], P(None, 'dp'), may hold values from 0 to 15
Outputs:
- grad_in: float32 [2, 12, 512, 4096], P(None, 'pipe', 'dp', 'tensor')
- grad_out: float32 [2, 12, 512, 4096], P(None, 'pipe', 'dp', 'tensor')
- leaving: bfloat16 [2, 12, 2048, 4096], P(None, 'pipe', 'dp', 'tensor')
The draws below stay inside these ranges and needn't reach their ends.
Inputs may be any that keep to these rules, and one draw needn't show every extreme that they name: `seq_lengths`: the 4 lengths of one microbatch on one replica sum to 128. `group_ids`: groups take sequences from several replicas and microbatches.
All inputs are finite; a program needn't handle non-finite values.
Results may differ from the reference program's by a relative error of at most 0.023.
Values may be sent and summed in bfloat16 or wider, within the bound.
A program may use at most 64 MiB of HBM per device.

```python
import math
import jax
import jax.numpy as jnp
import numpy as np
from jax import lax

D = 4096
R = 512
ROWS = 128
SEQS = 4
STEPS = 3
NEW = 2
GROUPS = 16
MOST = 64
N_PIPE = 12
N_DP = 16
N_TENSOR = 4


def set_ends(values, stream_key, smallest, top_value):
    place = [jax.random.randint(jax.random.fold_in(stream_key, axis), (), 0, length) for axis, length in enumerate(values.shape)]
    main_axis = values.shape.index(max(values.shape))
    next_to = place[:main_axis] + [(place[main_axis] + 1) % values.shape[main_axis]] + place[main_axis + 1:]
    return values.at[tuple(place)].set(smallest).at[tuple(next_to)].set(top_value)


def block_levels(own_key, shape, split, least, largest):
    gain = 1.0
    for axis_at, blocks in split:
        heights = jax.random.uniform(jax.random.fold_in(jax.random.fold_in(own_key, 6), axis_at), (blocks,), jnp.float32, least / len(split), largest / len(split))
        gain = gain * jnp.repeat(jnp.exp(heights), shape[axis_at] // blocks).reshape((-1,) + (1,) * (len(shape) - 1 - axis_at))
    return gain


def profile(number_of, total, bound, lean):
    loads = [(1 << 20) // math.isqrt(grade ** lean) + 1 for grade in range(2, number_of + 1)]
    spare, given = total - bound - (number_of - 1), [1] * (number_of - 1)
    while spare > 0:
        movable = [i for i in range(number_of - 1) if given[i] < bound]
        pool, budget = sum([loads[i] for i in movable]), spare
        for i in movable:
            extra = min(bound - given[i], max(1, budget * loads[i] // pool), spare)
            given[i] = given[i] + extra
            spare = spare - extra
    return np.array([bound] + given)


def ragged(own_key, count, total, reach, lean):
    if count == 2:
        one = jax.random.randint(own_key, (), max(1, total - reach), min(reach, total - 1) + 1)
        return jnp.stack([one, total - one])
    lengths = jnp.asarray(profile(count, total, reach, lean), jnp.int32)
    pairs = (count - 1) // 2
    source_of, sink = lengths[1:1 + 2 * pairs:2], lengths[2:2 + 2 * pairs:2]
    slack = jnp.minimum(source_of - 1, reach - sink)
    passed = jax.random.randint(jax.random.fold_in(own_key, 1), (pairs,), 0, 1 << 20) % (slack + 1)
    lengths = lengths.at[1:1 + 2 * pairs:2].set(source_of - passed).at[2:2 + 2 * pairs:2].set(sink + passed)
    return lengths[jax.random.permutation(jax.random.fold_in(own_key, 2), count)]


def normal_values(own_key, extent, spread, reach, shards=(), kind=jnp.bfloat16):
    gain = block_levels(own_key, extent, shards, -0.22, 0.18) if shards else 1.0
    entries = jax.random.normal(own_key, extent, jnp.float32) * spread * gain
    return jnp.minimum(jnp.maximum(entries, -reach), reach).astype(kind)


def setup_inputs(seed: int = 0) -> dict:
    streams_of = jax.random.split(jax.random.key(seed), 10)
    return {
        "saved_inputs": normal_values(streams_of[0], (STEPS, 2, N_PIPE, N_DP * ROWS, D), 1.0, 6.0, ((2, 12), (3, 16), (4, 4))),
        "proj_in": normal_values(streams_of[1], (2, N_PIPE, R, D), D ** -0.5, 0.09375, ((1, 12), (3, 4))),
        "proj_out": normal_values(streams_of[2], (2, N_PIPE, R, D), R ** -0.5, 0.25, ((1, 12), (3, 4))),
        "norm_gain": jnp.clip(1.0 + 0.18 * jax.random.normal(streams_of[3], (2, N_PIPE, D), jnp.float32), 0.1, 1.9),
        "arriving": normal_values(streams_of[4], (2, N_PIPE, N_DP * ROWS, D), 1.0, 6.0, ((1, 12), (2, 16), (3, 4))),
        "logp_grad": normal_values(streams_of[5], (NEW, N_DP * ROWS, D), 1.0, 6.0, ((1, 16), (2, 4))),
        "rewards": normal_values(streams_of[6], (NEW, N_DP, SEQS), 1.0, 4.0, ((1, 16),), jnp.float32),
        "seq_lengths": jax.vmap(lambda own: ragged(own, SEQS, ROWS, MOST, 2))(jax.random.split(streams_of[7], NEW * N_DP)).reshape((NEW, N_DP, SEQS)).astype(jnp.int32),
        "group_ids": set_ends(jax.random.randint(streams_of[8], (NEW, N_DP, SEQS), 0, GROUPS), jax.random.fold_in(streams_of[8], 1), 0, GROUPS - 1).astype(jnp.int32),
    }


EPS = 1e-05

def silu_slope(values):
    sigma = jax.nn.sigmoid(values)
    return sigma * (1.0 + values * (1.0 - sigma))

def round_trip(values):
    return lax.optimization_barrier(values.astype(jnp.bfloat16)).astype(jnp.float32)

def block_product(left, right):
    count = left.shape[0]
    width = right.shape[0]
    left_blocks = left.astype(jnp.float32).reshape(count, N_TENSOR, D // N_TENSOR)
    right_blocks = right.astype(jnp.float32).reshape(width, N_TENSOR, D // N_TENSOR)
    pieces = jnp.einsum('rtd,ktd->trk', left_blocks, right_blocks)
    return lax.optimization_barrier(jnp.sum(round_trip(pieces), axis=0))

def block_back(operands):
    inputs, arrive, weight_in, weight_out, gain_row = operands
    inputs_f = inputs.astype(jnp.float32)
    squares = lax.optimization_barrier(jnp.sum(inputs_f * inputs_f, axis=-1))
    inv_rms = 1.0 / jnp.sqrt(squares / D + EPS)
    gained = (inputs_f * gain_row).astype(jnp.bfloat16)
    pre_sum = block_product(gained, weight_in)
    back_sum = block_product(arrive, weight_out)
    pre_act = inv_rms[:, None] * pre_sum
    hidden = jax.nn.silu(pre_act).astype(jnp.bfloat16)
    grad_pre = back_sum * silu_slope(pre_act)
    grad_scaled = (inv_rms[:, None] * grad_pre).astype(jnp.bfloat16)
    grad_gained = jnp.dot(grad_scaled, weight_in, preferred_element_type=jnp.float32)
    radial_sum = lax.optimization_barrier(jnp.sum(grad_pre * pre_sum, axis=-1))
    out_cot = arrive.astype(jnp.float32) + gain_row * grad_gained - inputs_f * (inv_rms ** 3 * radial_sum / D)[:, None]
    return (out_cot.astype(jnp.bfloat16), grad_scaled, hidden)

def top_cotangent(logp_grad, rewards, seq_lengths, group_ids):
    groups = jnp.arange(GROUPS, dtype=jnp.int32)
    member = (group_ids[..., None] == groups).astype(jnp.float32)
    sums = lax.optimization_barrier(jnp.sum(member * rewards[..., None], axis=(0, 1, 2)))
    counts = lax.optimization_barrier(jnp.sum(member, axis=(0, 1, 2)))
    means = sums / jnp.maximum(counts, 1.0)
    advantage = rewards - lax.optimization_barrier(jnp.sum(member * means, axis=-1))
    ends = jnp.cumsum(seq_lengths, axis=-1).astype(jnp.int32)
    position = jnp.arange(ROWS, dtype=jnp.int32)
    segment = lax.optimization_barrier(jnp.sum((position[:, None] >= ends[..., None, :]).astype(jnp.int32), axis=-1))
    pick = (segment[..., None] == jnp.arange(SEQS, dtype=jnp.int32)).astype(jnp.float32)
    weights = lax.optimization_barrier(jnp.sum(pick * advantage[..., None, :], axis=-1)).reshape(NEW, N_DP * ROWS)
    return (-weights[..., None] * logp_grad.astype(jnp.float32)).astype(jnp.bfloat16)

def reference(saved_inputs, proj_in, proj_out, norm_gain, arriving, logp_grad, rewards, seq_lengths, group_ids):
    entering = top_cotangent(logp_grad, rewards, seq_lengths, group_ids)
    slots = 2 * N_PIPE
    tokens = N_DP * ROWS
    weights_in = proj_in.reshape(slots, R, D)
    weights_out = proj_out.reshape(slots, R, D)
    gains = norm_gain.reshape(slots, D)
    current = arriving
    cot_list = []
    scaled_list = []
    hidden_list = []
    out_cot = arriving
    for step_index in range(STEPS):
        inputs = saved_inputs[step_index].reshape(slots, tokens, D)
        flat_cot = current.reshape(slots, tokens, D)
        out_flat, grad_scaled, hidden = lax.map(block_back, (inputs, flat_cot, weights_in, weights_out, gains))
        cot_list.append(flat_cot)
        scaled_list.append(grad_scaled)
        hidden_list.append(hidden)
        out_cot = out_flat.reshape(2, N_PIPE, tokens, D)
        if step_index + 1 < STEPS:
            lower = jnp.concatenate([out_cot[0, 1:], out_cot[1, :1]], axis=0)
            upper = jnp.concatenate([out_cot[1, 1:], entering[step_index][None]], axis=0)
            current = jnp.stack([lower, upper])
    cot_all = jnp.stack(cot_list)
    scaled_all = jnp.stack(scaled_list)
    hidden_all = jnp.stack(hidden_list)
    saved_all = saved_inputs.reshape(STEPS, slots, tokens, D)
    scale = 1.0 / (N_DP * ROWS)

    def slot_grads(slot):
        slot = slot.astype(jnp.int32)
        inputs = lax.dynamic_index_in_dim(saved_all, slot, 1, keepdims=False)
        arrive = lax.dynamic_index_in_dim(cot_all, slot, 1, keepdims=False)
        grad_scaled = lax.dynamic_index_in_dim(scaled_all, slot, 1, keepdims=False)
        hidden = lax.dynamic_index_in_dim(hidden_all, slot, 1, keepdims=False)
        gain_row = lax.dynamic_index_in_dim(gains, slot, 0, keepdims=False)
        gained = (inputs.astype(jnp.float32) * gain_row).astype(jnp.bfloat16)
        left_in = grad_scaled.astype(jnp.float32).reshape(STEPS, N_DP, ROWS, R)
        right_in = gained.astype(jnp.float32).reshape(STEPS, N_DP, ROWS, D)
        per_in = jnp.einsum('snrk,snrd->nkd', left_in, right_in)
        left_out = hidden.astype(jnp.float32).reshape(STEPS, N_DP, ROWS, R)
        right_out = arrive.astype(jnp.float32).reshape(STEPS, N_DP, ROWS, D)
        per_out = jnp.einsum('snrk,snrd->nkd', left_out, right_out)
        total_in = lax.optimization_barrier(jnp.sum(round_trip(per_in), axis=0)) * scale
        total_out = lax.optimization_barrier(jnp.sum(round_trip(per_out), axis=0)) * scale
        return (total_in, total_out)
    grad_in, grad_out = lax.map(slot_grads, jnp.arange(slots, dtype=jnp.int32))
    return (grad_in.reshape(2, N_PIPE, R, D), grad_out.reshape(2, N_PIPE, R, D), out_cot)
```

```python
import jax
import jax.numpy as jnp
from jax import lax
from jax.experimental import pallas as pl
from jax.experimental.pallas import tpu as pltpu
from jax.sharding import PartitionSpec as P

D = 4096
EPS = 1e-05
ROWS = 128
HALF = 64
DL = 1024
R = 512
STEPS = 3
SEQS = 4
F32 = jnp.float32
BF16 = jnp.bfloat16
MESH = pl.DeviceIdType.MESH

SPLITS = ((0, 768, "x"), (768, 256, "y"))
N_SEM = 208


def slope_of(values, sigma):
    return sigma * (1.0 + values * (1.0 - sigma))


def dot_nt(a, b):
    return lax.dot_general(a, b, (((1,), (1,)), ((), ())), preferred_element_type=F32)


def dot_nn(a, b):
    return lax.dot_general(a, b, (((1,), (0,)), ((), ())), preferred_element_type=F32)


def dot_tn(a, b):
    return lax.dot_general(a, b, (((0,), (0,)), ((), ())), preferred_element_type=F32)


def kernel(
    sections,
    saved_hbm, win_hbm, wout_hbm, gain, arriving_hbm, logp_hbm, rewards, lengths, ids,
    gin_hbm, gout_hbm, leaving_hbm,
    xs, win, wout, lg, call, gained, hid, gs, coef,
    part_pre, part_back, d_pre, d_back, chip_pre, chip_back, y_pre, y_back,
    sq, sq_d, sq_chip, sq_y, inv, slope, presum, cout,
    rw, rw_x, rw_sum, rw_y, weight,
    g, h1, f1, s1, h2, f2, fin,
    load_sem, store_sem, send_sem, recv_sem,
):
    sec = lax.axis_index("pipe")
    dp = lax.axis_index("dp")
    tn = lax.axis_index("tensor")
    xi = dp // 4
    yi = dp % 4
    core = tn % 2
    mine = pl.multiple_of(core * HALF, HALF)
    other = pl.multiple_of((1 - core) * HALF, HALF)
    top = sec == sections - 1

    partner = (sec, dp, tn + 1 - 2 * core)
    across = (sec, dp, (tn + 2) % 4)
    below = ((sec + sections - 1) % sections, dp, tn)
    above = ((sec + 1) % sections, dp, tn)

    def at_x(by):
        return (sec, ((xi + by) % 4) * 4 + yi, tn)

    def at_y(by):
        return (sec, xi * 4 + (yi + by) % 4, tn)

    peers = [partner, across, below, above] + [at(by) for at in (at_x, at_y) for by in (1, 2, 3)]

    used = [0]
    sends = []

    def remote(src, dst, device):
        k = used[0]
        used[0] += 1
        copy = pltpu.make_async_remote_copy(
            src_ref=src, dst_ref=dst, send_sem=send_sem.at[k], recv_sem=recv_sem.at[k],
            device_id=device, device_id_type=MESH,
        )
        copy.start()
        sends.append(copy)
        return copy

    loads = {}

    def load(name, src, dst):
        copy = pltpu.make_async_copy(src, dst, load_sem.at[len(loads)])
        copy.start()
        loads[name] = copy

    for v in range(2):
        load(("c", v), arriving_hbm.at[v], call.at[v, pl.ds(0, ROWS)])
        load(("wout", v), wout_hbm.at[v], wout.at[v])
        load(("x", 0, v), saved_hbm.at[0, v], xs.at[0, v])
        load(("win", v), win_hbm.at[v], win.at[v])
    for t in (1, 2):
        for v in range(2):
            load(("x", t, v), saved_hbm.at[t, v], xs.at[t, v])
    load("lg", logp_hbm, lg)

    barrier = pltpu.get_barrier_semaphore()
    for peer in peers:
        pl.semaphore_signal(barrier, inc=1, device_id=peer, device_id_type=MESH)

    lane = lax.broadcasted_iota(jnp.int32, (8, 128), 1)
    row = lax.broadcasted_iota(jnp.int32, (8, 128), 0)
    tile = jnp.zeros((8, 128), F32)
    for n in range(2):
        for k in range(SEQS):
            member = lane == ids[n, 0, k]
            tile = tile + jnp.where(
                member, jnp.where(row == 0, rewards[n, 0, k], jnp.where(row == 1, 1.0, 0.0)), 0.0
            )
    rw[...] = tile

    rows_of = [pl.ds(t * ROWS, ROWS) for t in range(STEPS)]

    def back_part(t, v):
        for n in range(2):
            cols = pl.ds(n * 256, 256)
            part_back[t, v, :, cols] = dot_nt(
                call[v, rows_of[t], :], wout[v, cols, :]
            ).astype(BF16)

    def back_send(t, v):
        return remote(part_back.at[t, v, pl.ds(other, HALF)], d_back.at[t, v], partner)

    def pre_part(t, v):
        gain_row = gain[v]
        slot = 0 if t == 0 else 1
        lane_no = t * 2 + v

        def body(i, carry):
            r = pl.ds(pl.multiple_of(i * 16, 16), 16)
            values = xs[t, v, r, :].astype(F32)
            gained[v, pl.ds(pl.multiple_of(t * ROWS + i * 16, 16), 16), :] = (
                values * gain_row
            ).astype(BF16)
            total = jnp.sum(values * values, axis=-1, keepdims=True)
            at = lax.broadcasted_iota(jnp.int32, (16, 128), 1) == lane_no
            sq[slot, r, :] = jnp.where(at, total, sq[slot, r, :])
            return carry

        lax.fori_loop(0, ROWS // 16, body, 0)
        for n in range(2):
            cols = pl.ds(n * 256, 256)
            part_pre[t, v, :, cols] = dot_nt(
                gained[v, rows_of[t], :], win[v, cols, :]
            ).astype(BF16)

    def pre_send(t, v):
        return remote(part_pre.at[t, v, pl.ds(other, HALF)], d_pre.at[t, v], partner)

    def chip_sum(t, v, copy, part, arrived, chip, far):
        copy.wait_recv()
        chip[t, v] = (
            part[t, v, pl.ds(mine, HALF), :].astype(F32) + arrived[t, v].astype(F32)
        ).astype(BF16)
        return remote(chip.at[t, v], far.at[t, v], across)

    def sq_chip_sum(slot, copy):
        copy.wait_recv()
        sq_chip[slot] = sq[slot, pl.ds(mine, HALF), :] + sq_d[slot]
        return remote(sq_chip.at[slot], sq_y.at[slot], across)

    def inv_of(slot, copy):
        copy.wait_recv()
        total = sq_chip[slot] + sq_y[slot]
        inv[slot] = 1.0 / jnp.sqrt(total / D + EPS)

    def inv_rows(t, v, r):
        lane_no = t * 2 + v
        return inv[0 if t == 0 else 1, r, :][:, lane_no : lane_no + 1]

    def hidden_of(t, v, copy):
        copy.wait_recv()

        def body(i, carry):
            r = pl.ds(pl.multiple_of(i * 16, 16), 16)
            total = chip_pre[t, v, r, :].astype(F32) + y_pre[t, v, r, :].astype(F32)
            pre = inv_rows(t, v, r) * total
            sigma = jax.nn.sigmoid(pre)
            presum[t, v, r, :] = total
            slope[t, v, r, :] = slope_of(pre, sigma)
            where = pl.ds(pl.multiple_of(t * ROWS + mine + i * 16, 16), 16)
            hid[v, where, :] = (pre * sigma).astype(BF16)
            return carry

        lax.fori_loop(0, HALF // 16, body, 0)
        own = pl.ds(pl.multiple_of(t * ROWS + mine, HALF), HALF)
        return remote(hid.at[v, own], hid.at[v, own], partner)

    def scaled_of(t, v, copy):
        copy.wait_recv()

        def body(i, carry):
            r = pl.ds(pl.multiple_of(i * 16, 16), 16)
            back = chip_back[t, v, r, :].astype(F32) + y_back[t, v, r, :].astype(F32)
            scale = inv_rows(t, v, r)
            grad_pre = back * slope[t, v, r, :]
            where = pl.ds(pl.multiple_of(t * ROWS + mine + i * 16, 16), 16)
            gs[v, where, :] = (scale * grad_pre).astype(BF16)
            radial = jnp.sum(grad_pre * presum[t, v, r, :], axis=-1, keepdims=True)
            amount = scale * scale * scale * radial / D
            here = pl.ds(pl.multiple_of(mine + i * 16, 16), 16)
            coef[t, v, here, :] = jnp.broadcast_to(amount, (16, 128))
            return carry

        lax.fori_loop(0, HALF // 16, body, 0)
        own = pl.ds(pl.multiple_of(t * ROWS + mine, HALF), HALF)
        here = pl.ds(mine, HALF)
        return (
            remote(gs.at[v, own], gs.at[v, own], partner),
            remote(coef.at[t, v, here], coef.at[t, v, here], partner),
        )

    def cot_out(t, v, copies):
        for copy in copies:
            copy.wait_recv()
        amount = coef[t, v]
        for n in range(4):
            cols = pl.ds(n * 256, 256)
            product = dot_nn(gs[v, rows_of[t], :], win[v, :, cols])
            out = (
                call[v, rows_of[t], cols].astype(F32)
                + gain[v, :, cols] * product
                - xs[t, v, :, cols].astype(F32) * amount[:, :1]
            )
            cout[t, v, :, cols] = out.astype(BF16)

    def shift(t, v):
        k = t * 2 + v
        slot = v if v == 0 else jnp.where(sec == 0, 0, 1)
        copy = pltpu.make_async_remote_copy(
            src_ref=cout.at[t, v], dst_ref=call.at[slot, rows_of[t + 1]],
            send_sem=send_sem.at[N_SEM - 4 + k], recv_sem=recv_sem.at[N_SEM - 4 + t * 2 + slot],
            device_id=below, device_id_type=MESH,
        )
        if v == 1:
            copy.start()
        else:
            @pl.when(sec != 0)
            def _():
                copy.start()

        return copy

    def shift_in(t, v):
        slot_ref = call.at[v, rows_of[t + 1]]
        copy = pltpu.make_async_remote_copy(
            src_ref=slot_ref, dst_ref=slot_ref,
            send_sem=send_sem.at[N_SEM - 4 + t * 2 + v], recv_sem=recv_sem.at[N_SEM - 4 + t * 2 + v],
            device_id=below, device_id_type=MESH,
        )
        if v == 0:
            copy.wait_recv()
        else:
            @pl.when(jnp.logical_not(top))
            def _():
                copy.wait_recv()

    class Ring:
        def __init__(self, p, kind, v, first, width, axis):
            self.p, self.kind, self.v = p, kind, v
            self.cols = pl.ds(first, width)
            if axis == "x":
                self.axes = ((xi, at_x), (yi, at_y))
                self.chunk = lambda j, lo, n: g.at[p, j, pl.ds(lo, n), :, self.cols]
            else:
                self.axes = ((yi, at_y), (xi, at_x))
                self.chunk = lambda j, lo, n: g.at[p, pl.ds(lo, n), j, :, self.cols]

        def start(self, phase):
            i, at = self.axes[phase]
            nxt, prv = at(1), at(3)
            far, up, down = (i + 2) % 4, (i + 1) % 4, (i + 3) % 4
            c = self.cols
            if phase == 0:
                src, n = self.chunk, 2
                half = lambda d: h1.at[self.p, d, :, :, c]
                full = lambda d, lo: f1.at[self.p, d, pl.ds(lo, 2), :, c]
            else:
                src = lambda j, lo, n: s1.at[self.p, j, pl.ds(lo, n), c]
                n = 16
                half = lambda d: h2.at[self.p, d, :, c]
                full = lambda d, lo: f2.at[self.p, d, pl.ds(lo, 16), c]
            self.src, self.n, self.full = src, n, full
            self.half_a = remote(src(far, 0, n), half(0), nxt)
            self.half_b = remote(src(far, n, n), half(1), prv)
            self.plain = [
                remote(src(up, n, n), full(0, n), nxt),
                remote(src(down, 0, n), full(1, 0), prv),
            ]

        def merge(self, phase):
            i, at = self.axes[phase]
            nxt, prv = at(1), at(3)
            up, down = (i + 1) % 4, (i + 3) % 4
            n = self.n
            for d, copy, j, lo in ((0, self.half_a, up, 0), (1, self.half_b, down, n)):
                copy.wait_recv()
                chunk = self.src(j, lo, n)
                arrived = (h1 if phase == 0 else h2).at[self.p, d]
                if phase == 0:
                    arrived = arrived.at[:, :, self.cols]
                else:
                    arrived = arrived.at[:, self.cols]
                chunk[...] = (chunk[...].astype(F32) + arrived[...].astype(F32)).astype(BF16)
                self.plain.append(remote(chunk, self.full(d, lo), (nxt, prv)[d]))

        def middle(self):
            for copy in self.plain:
                copy.wait_recv()
            i = self.axes[0][0]
            for k in range(4):
                own = self.chunk(i, k, 1)
                total = own[...].reshape(32, -1).astype(F32)
                for d in range(2):
                    total = total + f1[self.p, d, k, :, self.cols].astype(F32)
                s1[self.p, k, :, self.cols] = total.astype(BF16)
            self.start(1)

        def end(self):
            for copy in self.plain:
                copy.wait_recv()
            i = self.axes[1][0]
            total = s1[self.p, i, :, self.cols].astype(F32)
            for d in range(2):
                total = total + f2[self.p, d, :, self.cols].astype(F32)
            fin[self.kind, self.v, :, self.cols] = total * (1.0 / (16 * ROWS))

    stores = []

    def store(src, dst):
        copy = pltpu.make_async_copy(src, dst, store_sem.at[len(stores)])
        copy.start()
        stores.append(copy)

    class Piece:
        def __init__(self, p, kind, v):
            self.p, self.kind, self.v = p, kind, v
            self.rings = [Ring(p, kind, v, *split) for split in SPLITS]

        def start(self):
            left, right = ((gs, gained), (hid, call))[self.kind]
            v, p = self.v, self.p

            def body(m, carry):
                j = (xi + 2 + m) % 4
                lhs = left[v, :, pl.ds(pl.multiple_of(j * 128, 128), 128)]
                for n in range(4):
                    cols = pl.ds(n * 256, 256)
                    block = dot_tn(lhs, right[v, :, cols]).astype(BF16)
                    g[p, j, :, :, cols] = block.reshape(4, 32, 256)
                return carry

            lax.fori_loop(0, 4, body, 0)
            for ring in self.rings:
                ring.start(0)

        def merge(self, phase):
            for ring in self.rings:
                ring.merge(phase)

        def middle(self):
            for ring in self.rings:
                ring.middle()

        def end(self):
            for ring in self.rings:
                ring.end()
            store(fin.at[self.kind, self.v], (gin_hbm, gout_hbm)[self.kind].at[self.v])

    loads[("c", 0)].wait()
    loads[("wout", 0)].wait()
    back_part(0, 0)
    pl.semaphore_wait(barrier, len(peers))
    pre_copy, back_copy, sq_copy = {}, {}, {}
    back_copy[0, 0] = back_send(0, 0)
    rw_copies = [remote(rw, rw_x.at[by - 1], at_x(by)) for by in (1, 2, 3)]
    sq[...] = jnp.zeros_like(sq)
    loads[("x", 0, 0)].wait()
    loads[("win", 0)].wait()
    pre_part(0, 0)
    pre_copy[0, 0] = pre_send(0, 0)
    loads[("c", 1)].wait()
    loads[("wout", 1)].wait()
    back_part(0, 1)
    back_copy[0, 1] = back_send(0, 1)
    loads[("x", 0, 1)].wait()
    loads[("win", 1)].wait()
    pre_part(0, 1)
    pre_copy[0, 1] = pre_send(0, 1)
    sq_copy[0] = remote(sq.at[0, pl.ds(other, HALF)], sq_d.at[0], partner)

    def back_chip(t, v):
        back_copy[t, v] = chip_sum(t, v, back_copy[t, v], part_back, d_back, chip_back, y_back)

    def pre_chip(t, v):
        pre_copy[t, v] = chip_sum(t, v, pre_copy[t, v], part_pre, d_pre, chip_pre, y_pre)

    back_chip(0, 0)
    pre_chip(0, 0)
    sq_copy[0] = sq_chip_sum(0, sq_copy[0])
    back_chip(0, 1)
    pre_chip(0, 1)
    for t in (1, 2):
        for v in range(2):
            loads[("x", t, v)].wait()
            pre_part(t, v)
            pre_copy[t, v] = pre_send(t, v)
    sq_copy[1] = remote(sq.at[1, pl.ds(other, HALF)], sq_d.at[1], partner)
    for copy in rw_copies:
        copy.wait_recv()
    rw_sum[...] = rw[...] + rw_x[0] + rw_x[1] + rw_x[2]
    rw_copies = [remote(rw_sum, rw_y.at[by - 1], at_y(by)) for by in (1, 2, 3)]

    inv_of(0, sq_copy[0])
    hid_copy, gs_copy = {}, {}
    for v in range(2):
        hid_copy[0, v] = hidden_of(0, v, pre_copy[0, v])
        gs_copy[0, v] = scaled_of(0, v, back_copy[0, v])
    shifts = []
    for v in range(2):
        cot_out(0, v, gs_copy[0, v])
        shifts.append(shift(0, v))

    sq_copy[1] = sq_chip_sum(1, sq_copy[1])
    for t in (1, 2):
        for v in range(2):
            pre_chip(t, v)
    loads["lg"].wait()
    for copy in rw_copies:
        copy.wait_recv()
    sums = rw_sum[...] + rw_y[0] + rw_y[1] + rw_y[2]
    means = sums[0:1, :] / jnp.maximum(sums[1:2, :], 1.0)
    position = lax.broadcasted_iota(jnp.int32, (ROWS, 128), 0)
    for n in range(2):
        begin = jnp.int32(0)
        weights = jnp.zeros((ROWS, 128), F32)
        for k in range(SEQS):
            finish = begin + lengths[n, 0, k]
            own = jnp.sum(
                jnp.where(lane[0:1, :] == ids[n, 0, k], means, 0.0), axis=-1, keepdims=True
            )
            advantage = rewards[n, 0, k] - own
            inside = jnp.logical_and(position >= begin, position < finish)
            weights = weights + jnp.where(inside, advantage, 0.0)
            begin = finish
        weight[n] = -weights

    @pl.when(top)
    def _():
        for n in range(2):
            def body(i, carry):
                r = pl.ds(pl.multiple_of(i * 16, 16), 16)
                to = pl.ds(pl.multiple_of((n + 1) * ROWS + i * 16, 16), 16)
                call[1, to, :] = (weight[n, r, :][:, :1] * lg[n, r, :].astype(F32)).astype(BF16)
                return carry

            lax.fori_loop(0, ROWS // 16, body, 0)

    inv_of(1, sq_copy[1])
    for t in (1, 2):
        for v in range(2):
            hid_copy[t, v] = hidden_of(t, v, pre_copy[t, v])

    for v in range(2):
        shift_in(0, v)
        back_part(1, v)
        back_copy[1, v] = back_send(1, v)
        back_chip(1, v)
        gs_copy[1, v] = scaled_of(1, v, back_copy[1, v])
        cot_out(1, v, gs_copy[1, v])
        shifts.append(shift(1, v))
    for t in range(STEPS):
        for v in range(2):
            hid_copy[t, v].wait_recv()

    out_piece = [Piece(0, 1, 0), Piece(2, 1, 1)]
    in_piece = [Piece(1, 0, 0), Piece(3, 0, 1)]

    shift_in(1, 0)
    back_part(2, 0)
    back_copy[2, 0] = back_send(2, 0)
    out_piece[0].start()
    back_chip(2, 0)
    gs_copy[2, 0] = scaled_of(2, 0, back_copy[2, 0])
    cot_out(2, 0, gs_copy[2, 0])
    store(cout.at[2, 0], leaving_hbm.at[0])
    in_piece[0].start()
    out_piece[0].merge(0)
    shift_in(1, 1)
    back_part(2, 1)
    back_copy[2, 1] = back_send(2, 1)
    out_piece[1].start()
    back_chip(2, 1)
    in_piece[0].merge(0)
    gs_copy[2, 1] = scaled_of(2, 1, back_copy[2, 1])
    cot_out(2, 1, gs_copy[2, 1])
    store(cout.at[2, 1], leaving_hbm.at[1])
    in_piece[1].start()
    out_piece[1].merge(0)
    out_piece[0].middle()
    in_piece[1].merge(0)
    out_piece[0].merge(1)
    in_piece[0].middle()
    in_piece[0].merge(1)
    out_piece[0].end()
    out_piece[1].middle()
    out_piece[1].merge(1)
    in_piece[0].end()
    in_piece[1].middle()
    in_piece[1].merge(1)
    out_piece[1].end()
    in_piece[1].end()

    for copy in sends:
        copy.wait_send()

    @pl.when(sec != 0)
    def _():
        shifts[0].wait_send()
        shifts[2].wait_send()

    shifts[1].wait_send()
    shifts[3].wait_send()
    for copy in stores:
        copy.wait()
    assert used[0] <= N_SEM - 4, used[0]


def shards(saved, proj_in, proj_out, gain, arriving, logp, rewards, lengths, ids):
    sections = lax.axis_size("pipe")
    any_spec = pl.BlockSpec(memory_space=pl.ANY)
    vmem = pl.BlockSpec(memory_space=pltpu.VMEM)
    smem = pl.BlockSpec(memory_space=pltpu.SMEM)
    V = pltpu.VMEM
    grad_in, grad_out, leaving = pl.pallas_call(
        lambda *refs: kernel(sections, *refs),
        name="window",
        out_shape=(
            jax.ShapeDtypeStruct((2, 32, DL), F32),
            jax.ShapeDtypeStruct((2, 32, DL), F32),
            jax.ShapeDtypeStruct((2, ROWS, DL), BF16),
        ),
        in_specs=[any_spec, any_spec, any_spec, vmem, any_spec, any_spec, smem, smem, smem],
        out_specs=(any_spec, any_spec, any_spec),
        scratch_shapes=[
            V((STEPS, 2, ROWS, DL), BF16),
            V((2, R, DL), BF16),
            V((2, R, DL), BF16),
            V((2, ROWS, DL), BF16),
            V((2, STEPS * ROWS, DL), BF16),
            V((2, STEPS * ROWS, DL), BF16),
            V((2, STEPS * ROWS, R), BF16),
            V((2, STEPS * ROWS, R), BF16),
            V((STEPS, 2, ROWS, 128), F32),
            V((STEPS, 2, ROWS, R), BF16),
            V((STEPS, 2, ROWS, R), BF16),
            V((STEPS, 2, HALF, R), BF16),
            V((STEPS, 2, HALF, R), BF16),
            V((STEPS, 2, HALF, R), BF16),
            V((STEPS, 2, HALF, R), BF16),
            V((STEPS, 2, HALF, R), BF16),
            V((STEPS, 2, HALF, R), BF16),
            V((2, ROWS, 128), F32),
            V((2, HALF, 128), F32),
            V((2, HALF, 128), F32),
            V((2, HALF, 128), F32),
            V((2, HALF, 128), F32),
            V((STEPS, 2, HALF, R), F32),
            V((STEPS, 2, HALF, R), F32),
            V((STEPS, 2, ROWS, DL), BF16),
            V((8, 128), F32),
            V((3, 8, 128), F32),
            V((8, 128), F32),
            V((3, 8, 128), F32),
            V((2, ROWS, 128), F32),
            V((4, 4, 4, 32, DL), BF16),
            V((4, 2, 2, 32, DL), BF16),
            V((4, 2, 4, 32, DL), BF16),
            V((4, 4, 32, DL), BF16),
            V((4, 2, 16, DL), BF16),
            V((4, 2, 32, DL), BF16),
            V((2, 2, 32, DL), F32),
            pltpu.SemaphoreType.DMA((16,)),
            pltpu.SemaphoreType.DMA((8,)),
            pltpu.SemaphoreType.DMA((N_SEM,)),
            pltpu.SemaphoreType.DMA((N_SEM,)),
        ],
        compiler_params=pltpu.CompilerParams(
            collective_id=0, has_side_effects=True, vmem_limit_bytes=60 * 2**20
        ),
    )(
        saved[:, :, 0], proj_in[:, 0], proj_out[:, 0], gain, arriving[:, 0], logp,
        rewards, lengths, ids,
    )
    return grad_in[:, None], grad_out[:, None], leaving[:, None]


def solution(mesh):
    return jax.shard_map(
        shards,
        mesh=mesh,
        in_specs=(
            P(None, None, "pipe", "dp", "tensor"),
            P(None, "pipe", None, "tensor"),
            P(None, "pipe", None, "tensor"),
            P(None, "pipe", "tensor"),
            P(None, "pipe", "dp", "tensor"),
            P(None, "dp", "tensor"),
            P(None, "dp", None),
            P(None, "dp", None),
            P(None, "dp", None),
        ),
        out_specs=(
            P(None, "pipe", "dp", "tensor"),
            P(None, "pipe", "dp", "tensor"),
            P(None, "pipe", "dp", "tensor"),
        ),
        check_vma=False,
    )
```

```python
import jax
import jax.numpy as jnp
from jax import lax
from jax.experimental import pallas as pl
from jax.experimental.pallas import tpu as pltpu
from jax.sharding import PartitionSpec as P

D = 4096
EPS = 1e-05
ROWS = 128
HALF = 64
DL = 1024
R = 512
STEPS = 3
SEQS = 4
F32 = jnp.float32
BF16 = jnp.bfloat16
MESH = pl.DeviceIdType.MESH

SPLITS = ((0, 768, "x"), (768, 256, "y"))
N_RECV = 96
N_SEND = 32
scope = jax.named_scope


def dot_nt(a, b):
    return lax.dot_general(a, b, (((1,), (1,)), ((), ())), preferred_element_type=F32)


def dot_nn(a, b):
    return lax.dot_general(a, b, (((1,), (0,)), ((), ())), preferred_element_type=F32)


def dot_tn(a, b):
    return lax.dot_general(a, b, (((0,), (0,)), ((), ())), preferred_element_type=F32)


def kernel(
    sections,
    saved_hbm, win_hbm, wout_hbm, gain_hbm, arriving_hbm, logp_hbm, rewards_hbm, lengths_hbm, ids_hbm,
    gin, gout, leaving,
    xs, win, wout, gain, lg, call, gained, hid, gs, coef,
    part_pre, part_back, d_pre, d_back, chip_pre, chip_back, y_pre, y_back,
    sqp, sq, sq_d, sq_chip, sq_y, inv, slope, presum, cout,
    rw, rw_in, weight, rewards, lengths, ids,
    g, h1, f1, s1, h2, f2,
    load_sem, send_sem, recv_sem, shift_send, shift_recv,
):
    sec = lax.axis_index("pipe")
    dp = lax.axis_index("dp")
    tn = lax.axis_index("tensor")
    xi = dp // 4
    yi = dp % 4
    core = tn % 2
    mine = pl.multiple_of(core * HALF, HALF)
    other = pl.multiple_of((1 - core) * HALF, HALF)
    top = sec == sections - 1
    early = [jnp.where(sec == 0, 1 - a, a) for a in range(2)]
    late = [jnp.where(top, 1 - a, a) for a in range(2)]
    block = [early, early, late]

    partner = (sec, dp, tn + 1 - 2 * core)
    across = (sec, dp, (tn + 2) % 4)
    below = ((sec + sections - 1) % sections, dp, tn)
    above = ((sec + 1) % sections, dp, tn)

    def at_x(to):
        return (sec, to * 4 + yi, tn)

    def at_y(to):
        return (sec, xi * 4 + to, tn)

    def ring(i, by):
        return (i + by) % 4

    peers = [partner, across, below, above]
    peers += [at_x(ring(xi, 1)), at_x(ring(xi, 3)), at_y(ring(yi, 1)), at_y(ring(yi, 3))]
    barrier = pltpu.get_barrier_semaphore()
    for peer in peers:
        pl.semaphore_signal(barrier, inc=1, device_id=peer, device_id_type=MESH)

    recv_used = [0]
    classes = {}

    def recv_slot():
        recv_used[0] += 1
        return recv_sem.at[recv_used[0] - 1]

    def send_slot(name, whole):
        if name not in classes:
            classes[name] = (send_sem.at[len(classes)], whole)
        return classes[name][0]

    def remote(src, dst, device, name, whole, recv=None):
        copy = pltpu.make_async_remote_copy(
            src_ref=src, dst_ref=dst, send_sem=send_slot(name, whole),
            recv_sem=recv_slot() if recv is None else recv,
            device_id=device, device_id_type=MESH,
        )
        copy.start()
        return copy

    def arrived(whole, recv):
        pltpu.make_async_remote_copy(
            src_ref=whole, dst_ref=whole, send_sem=send_sem.at[0], recv_sem=recv,
            device_id=partner, device_id_type=MESH,
        ).wait_recv()

    loads = {}

    def load(name, src, dst):
        copy = pltpu.make_async_copy(src, dst, load_sem.at[len(loads)])
        copy.start()
        loads[name] = copy

    load("gain", gain_hbm, gain)
    for a in range(2):
        v = early[a]
        load(("x", 0, a), saved_hbm.at[0, v], xs.at[0, v])
        load(("win", a), win_hbm.at[v], win.at[v])
        load(("c", a), arriving_hbm.at[v], call.at[v, pl.ds(0, ROWS)])
        load(("wout", a), wout_hbm.at[v], wout.at[v])
    for t in (1, 2):
        for a in range(2):
            load(("x", t, a), saved_hbm.at[t, block[t][a]], xs.at[t, block[t][a]])
    load("rewards", rewards_hbm, rewards)
    load("lengths", lengths_hbm, lengths)
    load("ids", ids_hbm, ids)
    load("lg", logp_hbm, lg)

    rows_of = [pl.ds(t * ROWS, ROWS) for t in range(STEPS)]

    def sixteen(start):
        return pl.ds(pl.multiple_of(start, 16), 16)

    back_copy, pre_copy, sq_copy, hid_copy, gs_copy = {}, {}, {}, {}, {}

    def back_part(t, a):
        v = block[t][a]
        with scope(f"back_part{t}{a}"):
            for n in range(2):
                cols = pl.ds(n * 256, 256)
                part_back[t, a, :, cols] = dot_nt(
                    call[v, rows_of[t], :], wout[v, cols, :]
                ).astype(BF16)

    def back_send(t, a):
        back_copy[t, a] = remote(
            part_back.at[t, a, pl.ds(other, HALF)], d_back.at[t, a], partner, "back", d_back
        )

    def pre_part(t, a):
        v = block[t][a]
        with scope(f"pre_part{t}{a}"):
            gain_row = gain[v]

            def body(i, carry):
                values = xs[t, v, sixteen(i * 16), :].astype(F32)
                gained[v, sixteen(t * ROWS + i * 16), :] = (values * gain_row).astype(BF16)
                squares = values * values
                part = squares[:, 0:128]
                for k in range(1, DL // 128):
                    part = part + squares[:, k * 128 : (k + 1) * 128]
                sqp[sixteen(i * 16), :] = part
                return carry

            lax.fori_loop(0, ROWS // 16, body, 0, unroll=2)
            for n in range(2):
                cols = pl.ds(n * 256, 256)
                part_pre[t, a, :, cols] = dot_nt(
                    gained[v, rows_of[t], :], win[v, cols, :]
                ).astype(BF16)
            total = jnp.sum(sqp[...], axis=-1, keepdims=True)
            same = lax.broadcasted_iota(jnp.int32, (ROWS, 128), 0) == lax.broadcasted_iota(
                jnp.int32, (ROWS, 128), 1
            )
            row = jnp.sum(jnp.where(same, total, 0.0), axis=0, keepdims=True)
            sq[t, a] = jnp.broadcast_to(row, (8, 128))

    def pre_send(t, a):
        pre_copy[t, a] = remote(
            part_pre.at[t, a, pl.ds(other, HALF)], d_pre.at[t, a], partner, "pre", d_pre
        )
        sq_copy[t, a] = remote(sq.at[t, a], sq_d.at[t, a], partner, "sq", sq_d)

    def chip_sum(t, a, copy, part, came, chip, far, name):
        copy.wait_recv()
        chip[t, a] = (
            part[t, a, pl.ds(mine, HALF), :].astype(F32) + came[t, a].astype(F32)
        ).astype(BF16)
        return remote(chip.at[t, a], far.at[t, a], across, name, far)

    def back_chip(t, a):
        with scope(f"back_chip{t}{a}"):
            back_copy[t, a] = chip_sum(
                t, a, back_copy[t, a], part_back, d_back, chip_back, y_back, "far_back"
            )

    def pre_chip(t, a):
        with scope(f"pre_chip{t}{a}"):
            pre_copy[t, a] = chip_sum(
                t, a, pre_copy[t, a], part_pre, d_pre, chip_pre, y_pre, "far_pre"
            )
            sq_copy[t, a].wait_recv()
            sq_chip[t, a] = sq[t, a] + sq_d[t, a]
            sq_copy[t, a] = remote(sq_chip.at[t, a], sq_y.at[t, a], across, "far_sq", sq_y)

    def hidden_of(t, a):
        v = block[t][a]
        with scope(f"hid_wait{t}{a}"):
            sq_copy[t, a].wait_recv()
            pre_copy[t, a].wait_recv()
        with scope(f"hidden{t}{a}"):
            total = sq_chip[t, a] + sq_y[t, a]
            inv_row = (1.0 / jnp.sqrt(total / D + EPS))[0:1, :]
            lane = lax.broadcasted_iota(jnp.int32, (HALF, 128), 1)
            line = lax.broadcasted_iota(jnp.int32, (HALF, 128), 0)
            scale = jnp.sum(jnp.where(lane == line + mine, inv_row, 0.0), axis=-1, keepdims=True)
            inv[t, a] = jnp.broadcast_to(scale, (HALF, 128))

            def body(i, carry):
                r = sixteen(i * 16)
                total = chip_pre[t, a, r, :].astype(F32) + y_pre[t, a, r, :].astype(F32)
                pre = inv[t, a, r, 0:1] * total
                sigma = jax.nn.sigmoid(pre)
                presum[t, a, r, :] = total
                slope[t, a, r, :] = sigma * (1.0 + pre * (1.0 - sigma))
                hid[v, sixteen(t * ROWS + mine + i * 16), :] = (pre * sigma).astype(BF16)
                return carry

            lax.fori_loop(0, HALF // 16, body, 0, unroll=True)
            own = pl.ds(pl.multiple_of(t * ROWS + mine, HALF), HALF)
            hid_copy[t, a] = remote(hid.at[v, own], hid.at[v, own], partner, "hid", d_pre)

    def scaled_of(t, a):
        v = block[t][a]
        with scope(f"gs_wait{t}{a}"):
            back_copy[t, a].wait_recv()
        with scope(f"scaled{t}{a}"):

            def body(i, carry):
                r = sixteen(i * 16)
                back = chip_back[t, a, r, :].astype(F32) + y_back[t, a, r, :].astype(F32)
                scale = inv[t, a, r, 0:1]
                grad_pre = back * slope[t, a, r, :]
                gs[v, sixteen(t * ROWS + mine + i * 16), :] = (scale * grad_pre).astype(BF16)
                radial = jnp.sum(grad_pre * presum[t, a, r, :], axis=-1, keepdims=True)
                amount = scale * scale * scale * radial / D
                coef[t, a, sixteen(mine + i * 16), :] = jnp.broadcast_to(amount, (16, 128))
                return carry

            lax.fori_loop(0, HALF // 16, body, 0, unroll=True)
            own = pl.ds(pl.multiple_of(t * ROWS + mine, HALF), HALF)
            here = pl.ds(mine, HALF)
            gs_copy[t, a] = (
                remote(gs.at[v, own], gs.at[v, own], partner, "gs", d_pre),
                remote(
                    coef.at[t, a, here], coef.at[t, a, here], partner, "coef",
                    coef.at[:, :, pl.ds(0, HALF)],
                ),
            )

    def gs_wait(t, a):
        with scope(f"gs_come{t}{a}"):
            for copy in gs_copy[t, a]:
                copy.wait_recv()

    def cot_out(t, a):
        v = block[t][a]
        with scope(f"cot_out{t}{a}"):
            amount = coef[t, a]
            for n in range(4):
                cols = pl.ds(n * 256, 256)
                product = dot_nn(gs[v, rows_of[t], :], win[v, :, cols])
                out = (
                    call[v, rows_of[t], cols].astype(F32)
                    + gain[v, :, cols] * product
                    - xs[t, v, :, cols].astype(F32) * amount[:, :1]
                ).astype(BF16)
                if t < STEPS - 1:
                    cout[t, a, :, cols] = out
                else:
                    leaving[v, :, cols] = out

    def shift_copy(t, a):
        return pltpu.make_async_remote_copy(
            src_ref=cout.at[t, a], dst_ref=call.at[a, rows_of[t + 1]],
            send_sem=shift_send.at[t * 2 + a], recv_sem=shift_recv.at[t * 2 + a],
            device_id=below, device_id_type=MESH,
        )

    def shift(t, a):
        if a == 0:
            shift_copy(t, a).start()
        else:
            @pl.when(sec != 0)
            def _():
                shift_copy(t, a).start()

    def shift_in(t, a):
        v = block[t][a]
        with scope(f"shift_in{t}{a}"):

            @pl.when(jnp.logical_not(jnp.logical_and(top, v == 1)))
            def _():
                arrived(call.at[v, rows_of[t]], shift_recv.at[(t - 1) * 2 + v])

    class Ring:
        def __init__(self, p, out, v, first, width, axis):
            self.p, self.out, self.v = p, out, v
            self.first, self.width = first, width
            self.name = f"{p}{axis}"
            cols = self.cols = pl.ds(first, width)
            pair = ((xi, at_x), (yi, at_y))
            if axis == "x":
                self.axes = pair
                chunk = lambda j, lo, n: g.at[p, j, pl.ds(lo, n), :, cols]
            else:
                self.axes = pair[::-1]
                chunk = lambda j, lo, n: g.at[p, pl.ds(lo, n), j, :, cols]
            small = lambda j, lo, n: s1.at[p, j, pl.ds(lo, n), cols]
            self.chunk = (chunk, small)
            self.n = (2, 16)
            self.half = (h1.at[p, :, :, :, cols], h2.at[p, :, :, cols])
            self.full = (f1.at[p, :, :, :, cols], f2.at[p, :, :, cols])
            self.half_recv = [recv_slot() for _ in range(2)]
            self.full_recv = [recv_slot() for _ in range(2)]

        def go(self, phase, j, lo, d, full):
            i, at = self.axes[phase]
            n = self.n[phase]
            src = self.chunk[phase](j, lo, n)
            to = at(ring(i, (1, 3)[d]))
            if full:
                dst = self.full[phase].at[d, pl.ds(lo, n)]
                remote(src, dst, to, f"f{phase}", (f1, f2)[phase], self.full_recv[phase])
            else:
                dst = self.half[phase].at[d]
                remote(src, dst, to, f"h{phase}", (h1, h2)[phase], self.half_recv[phase])

        def h(self, phase):
            far, n = ring(self.axes[phase][0], 2), self.n[phase]
            self.go(phase, far, 0, 0, False)
            self.go(phase, far, n, 1, False)

        def f(self, phase):
            i, n = self.axes[phase][0], self.n[phase]
            self.go(phase, ring(i, 1), n, 0, True)
            self.go(phase, ring(i, 3), 0, 1, True)

        def m(self, phase):
            i, n = self.axes[phase][0], self.n[phase]
            with scope(f"m{phase}_{self.name}"):
                arrived(self.half[phase], self.half_recv[phase])
                for d, j, lo in ((0, ring(i, 1), 0), (1, ring(i, 3), n)):
                    chunk = self.chunk[phase](j, lo, n)
                    came = self.half[phase].at[d]
                    chunk[...] = (chunk[...].astype(F32) + came[...].astype(F32)).astype(BF16)
                    self.go(phase, j, lo, d, True)

        def middle(self):
            with scope(f"mid_{self.name}"):
                arrived(self.full[0], self.full_recv[0])
                i = self.axes[0][0]
                for k in range(4):
                    total = self.chunk[0](i, k, 1)[...].reshape(32, self.width).astype(F32)
                    for d in range(2):
                        total = total + f1[self.p, d, k, :, self.cols].astype(F32)
                    s1[self.p, k, :, self.cols] = total.astype(BF16)
                self.h(1)
                self.f(1)

        def end(self):
            with scope(f"end_{self.name}"):
                arrived(self.full[1], self.full_recv[1])
                total = s1[self.p, self.axes[1][0], :, self.cols].astype(F32)
                for d in range(2):
                    total = total + f2[self.p, d, :, self.cols].astype(F32)
                self.out[self.v, :, self.cols] = total * (1.0 / (16 * ROWS))

    def piece(p, out, left, right, a):
        v = block[2][a]
        rings = [Ring(p, out, v, *split) for split in SPLITS]

        def compute(ring_):
            with scope(f"grad_{ring_.name}"):
                lhs = left[v]
                for k in range(ring_.width // 256):
                    cols = pl.ds(ring_.first + k * 256, 256)
                    made = dot_tn(lhs, right[v, :, cols]).astype(BF16)
                    g[p, :, :, :, cols] = made.reshape(4, 4, 32, 256)

        for ring_ in rings:
            ring_.compute = lambda ring_=ring_: compute(ring_)
        return rings

    loads["gain"].wait()
    loads[("x", 0, 0)].wait()
    loads[("win", 0)].wait()
    pre_part(0, 0)
    loads[("c", 0)].wait()
    loads[("wout", 0)].wait()
    back_part(0, 0)
    with scope("barrier"):
        pl.semaphore_wait(barrier, len(peers))
    pre_send(0, 0)
    back_send(0, 0)
    loads[("x", 0, 1)].wait()
    loads[("win", 1)].wait()
    pre_part(0, 1)
    pre_send(0, 1)
    pre_chip(0, 0)
    back_chip(0, 0)
    loads[("c", 1)].wait()
    loads[("wout", 1)].wait()
    back_part(0, 1)
    back_send(0, 1)
    pre_chip(0, 1)

    for name in ("rewards", "lengths", "ids"):
        loads[name].wait()
    lane = lax.broadcasted_iota(jnp.int32, (8, 128), 1)
    line = lax.broadcasted_iota(jnp.int32, (8, 128), 0)
    tile = jnp.zeros((8, 128), F32)
    for n in range(2):
        for k in range(SEQS):
            member = lane == ids[n, 0, k]
            amount = jnp.where(line == 0, rewards[n, 0, k], jnp.where(line == 1, 1.0, 0.0))
            tile = tile + jnp.where(member, amount, 0.0)
    rw[0] = tile
    partners = [at_x(xi + 1 - 2 * (xi % 2)), at_x(3 - xi), at_y(yi + 1 - 2 * (yi % 2)), at_y(3 - yi)]

    def rw_send(k):
        return remote(rw.at[k], rw_in.at[k], partners[k], "rw", rw_in)

    def rw_add(k, copy):
        copy.wait_recv()
        rw[k + 1] = rw[k] + rw_in[k]

    rw_copy = rw_send(0)
    back_chip(0, 1)
    loads[("x", 1, 0)].wait()
    pre_part(1, 0)
    pre_send(1, 0)
    hidden_of(0, 0)
    scaled_of(0, 0)
    pre_chip(1, 0)
    gs_wait(0, 0)
    cot_out(0, 0)
    shift(0, 0)
    rw_add(0, rw_copy)
    rw_copy = rw_send(1)
    loads[("x", 1, 1)].wait()
    pre_part(1, 1)
    pre_send(1, 1)
    hidden_of(0, 1)
    scaled_of(0, 1)
    pre_chip(1, 1)
    gs_wait(0, 1)
    cot_out(0, 1)
    shift(0, 1)

    rw_add(1, rw_copy)
    rw_copy = rw_send(2)
    for a in range(2):
        loads[("x", 2, a)].wait()
        pre_part(2, a)
        pre_send(2, a)
    hidden_of(1, 0)
    rw_add(2, rw_copy)
    rw_copy = rw_send(3)
    pre_chip(2, 0)
    pre_chip(2, 1)
    hidden_of(1, 1)
    loads["lg"].wait()
    rw_add(3, rw_copy)
    with scope("entering"):

        @pl.when(top)
        def _():
            sums = rw[4]
            means = sums[0:1, :] / jnp.maximum(sums[1:2, :], 1.0)
            position = lax.broadcasted_iota(jnp.int32, (ROWS, 128), 0)
            for n in range(2):
                begin = jnp.int32(0)
                weights = jnp.zeros((ROWS, 128), F32)
                for k in range(SEQS):
                    finish = begin + lengths[n, 0, k]
                    own = jnp.sum(
                        jnp.where(lane[0:1, :] == ids[n, 0, k], means, 0.0), axis=-1, keepdims=True
                    )
                    advantage = rewards[n, 0, k] - own
                    inside = jnp.logical_and(position >= begin, position < finish)
                    weights = weights + jnp.where(inside, advantage, 0.0)
                    begin = finish
                weight[n] = -weights

                def body(i, carry):
                    r = sixteen(i * 16)
                    values = weight[n, r, 0:1] * lg[n, r, :].astype(F32)
                    call[1, sixteen((n + 1) * ROWS + i * 16), :] = values.astype(BF16)
                    return carry

                lax.fori_loop(0, ROWS // 16, body, 0)

    shift_in(1, 0)
    back_part(1, 0)
    back_send(1, 0)
    hidden_of(2, 0)
    back_chip(1, 0)
    scaled_of(1, 0)
    gs_wait(1, 0)
    cot_out(1, 0)
    shift(1, 0)
    shift_in(1, 1)
    back_part(1, 1)
    back_send(1, 1)
    hidden_of(2, 1)
    back_chip(1, 1)
    scaled_of(1, 1)
    gs_wait(1, 1)
    cot_out(1, 1)
    shift(1, 1)
    for t in range(STEPS):
        for a in range(2):
            hid_copy[t, a].wait_recv()

    out0x, out0y = piece(0, gout, hid, call, 0)
    in0x, in0y = piece(1, gin, gs, gained, 0)
    out1x, out1y = piece(2, gout, hid, call, 1)
    in1x, in1y = piece(3, gin, gs, gained, 1)

    shift_in(2, 0)
    back_part(2, 0)
    back_send(2, 0)
    out0x.compute()
    out0x.h(0)
    out0x.f(0)
    back_chip(2, 0)
    out0y.compute()
    out0y.h(0)
    out0y.f(0)
    scaled_of(2, 0)
    shift_in(2, 1)
    back_part(2, 1)
    back_send(2, 1)
    out0x.m(0)
    gs_wait(2, 0)
    in0x.compute()
    in0x.h(0)
    out0y.m(0)
    back_chip(2, 1)
    in0y.compute()
    in0y.h(0)
    out1x.compute()
    in0x.f(0)
    out1x.h(0)
    out1y.compute()
    in0y.f(0)
    out1y.h(0)
    cot_out(2, 0)
    out0x.middle()
    out0y.middle()
    in0x.m(0)
    in0y.m(0)
    out1x.f(0)
    out1y.f(0)
    scaled_of(2, 1)
    gs_wait(2, 1)
    in1x.compute()
    in1x.h(0)
    in1y.compute()
    in1y.h(0)
    cot_out(2, 1)
    out1x.m(0)
    out1y.m(0)
    in1x.f(0)
    in1y.f(0)
    out0x.m(1)
    out0y.m(1)
    in0x.middle()
    in0y.middle()
    in1x.m(0)
    in1y.m(0)
    out0x.end()
    out0y.end()
    in0x.m(1)
    in0y.m(1)
    out1x.middle()
    out1y.middle()
    in0x.end()
    in0y.end()
    out1x.m(1)
    out1y.m(1)
    in1x.middle()
    in1y.middle()
    out1x.end()
    out1y.end()
    in1x.m(1)
    in1y.m(1)
    in1x.end()
    in1y.end()

    with scope("ends"):
        for sem, whole in classes.values():
            pltpu.make_async_remote_copy(
                src_ref=whole, dst_ref=whole, send_sem=sem, recv_sem=recv_sem.at[0],
                device_id=partner, device_id_type=MESH,
            ).wait_send()

        @pl.when(sec != 0)
        def _():
            shift_copy(0, 1).wait_send()
            shift_copy(1, 1).wait_send()

        shift_copy(0, 0).wait_send()
        shift_copy(1, 0).wait_send()
    assert recv_used[0] <= N_RECV and len(classes) <= N_SEND


def finish(gin, gout, leaving, gin_hbm, gout_hbm, leaving_hbm, sem):
    pairs = ((leaving, leaving_hbm), (gin, gin_hbm), (gout, gout_hbm))
    copies = [pltpu.make_async_copy(src, dst, sem.at[k]) for k, (src, dst) in enumerate(pairs)]
    for copy in copies:
        copy.start()
    for copy in copies:
        copy.wait()


def shards(saved, proj_in, proj_out, gain, arriving, logp, rewards, lengths, ids):
    sections = lax.axis_size("pipe")
    hbm = pl.BlockSpec(memory_space=pltpu.HBM)
    vmem = pl.BlockSpec(memory_space=pltpu.VMEM)
    V = pltpu.VMEM
    shapes = (
        jax.ShapeDtypeStruct((2, 32, DL), F32),
        jax.ShapeDtypeStruct((2, 32, DL), F32),
        jax.ShapeDtypeStruct((2, ROWS, DL), BF16),
    )
    results = pl.pallas_call(
        lambda *refs: kernel(sections, *refs),
        name="window",
        out_shape=shapes,
        in_specs=[hbm] * 9,
        out_specs=(vmem, vmem, vmem),
        scratch_shapes=[
            V((STEPS, 2, ROWS, DL), BF16),
            V((2, R, DL), BF16),
            V((2, R, DL), BF16),
            V((2, 1, DL), F32),
            V((2, ROWS, DL), BF16),
            V((2, STEPS * ROWS, DL), BF16),
            V((2, STEPS * ROWS, DL), BF16),
            V((2, STEPS * ROWS, R), BF16),
            V((2, STEPS * ROWS, R), BF16),
            V((STEPS, 2, ROWS, 128), F32),
            V((STEPS, 2, ROWS, R), BF16),
            V((STEPS, 2, ROWS, R), BF16),
            V((STEPS, 2, HALF, R), BF16),
            V((STEPS, 2, HALF, R), BF16),
            V((STEPS, 2, HALF, R), BF16),
            V((STEPS, 2, HALF, R), BF16),
            V((STEPS, 2, HALF, R), BF16),
            V((STEPS, 2, HALF, R), BF16),
            V((ROWS, 128), F32),
            V((STEPS, 2, 8, 128), F32),
            V((STEPS, 2, 8, 128), F32),
            V((STEPS, 2, 8, 128), F32),
            V((STEPS, 2, 8, 128), F32),
            V((STEPS, 2, HALF, 128), F32),
            V((STEPS, 2, HALF, R), F32),
            V((STEPS, 2, HALF, R), F32),
            V((STEPS - 1, 2, ROWS, DL), BF16),
            V((5, 8, 128), F32),
            V((4, 8, 128), F32),
            V((2, ROWS, 128), F32),
            pltpu.SMEM((2, 1, SEQS), F32),
            pltpu.SMEM((2, 1, SEQS), jnp.int32),
            pltpu.SMEM((2, 1, SEQS), jnp.int32),
            V((4, 4, 4, 32, DL), BF16),
            V((4, 2, 2, 32, DL), BF16),
            V((4, 2, 4, 32, DL), BF16),
            V((4, 4, 32, DL), BF16),
            V((4, 2, 16, DL), BF16),
            V((4, 2, 32, DL), BF16),
            pltpu.SemaphoreType.DMA((20,)),
            pltpu.SemaphoreType.DMA((N_SEND,)),
            pltpu.SemaphoreType.DMA((N_RECV,)),
            pltpu.SemaphoreType.DMA((4,)),
            pltpu.SemaphoreType.DMA((4,)),
        ],
        compiler_params=pltpu.CompilerParams(
            collective_id=0, has_side_effects=True, vmem_limit_bytes=40 * 2**20
        ),
    )(
        *(
            pltpu.with_memory_space_constraint(x, pltpu.HBM)
            for x in (
                saved[:, :, 0], proj_in[:, 0], proj_out[:, 0], gain, arriving[:, 0], logp,
                rewards, lengths, ids,
            )
        )
    )
    any_spec = pl.BlockSpec(memory_space=pl.ANY)
    results = pl.pallas_call(
        finish,
        name="finish",
        out_shape=shapes,
        in_specs=[vmem] * 3,
        out_specs=(any_spec,) * 3,
        scratch_shapes=[pltpu.SemaphoreType.DMA((3,))],
        compiler_params=pltpu.CompilerParams(vmem_limit_bytes=2**20),
    )(*results)
    return tuple(r[:, None] for r in results)


def solution(mesh):
    return jax.shard_map(
        shards,
        mesh=mesh,
        in_specs=(
            P(None, None, "pipe", "dp", "tensor"),
            P(None, "pipe", None, "tensor"),
            P(None, "pipe", None, "tensor"),
            P(None, "pipe", "tensor"),
            P(None, "pipe", "dp", "tensor"),
            P(None, "dp", "tensor"),
            P(None, "dp", None),
            P(None, "dp", None),
            P(None, "dp", None),
        ),
        out_specs=(
            P(None, "pipe", "dp", "tensor"),
            P(None, "pipe", "dp", "tensor"),
            P(None, "pipe", "dp", "tensor"),
        ),
        check_vma=False,
    )
```

```python
import jax
import jax.numpy as jnp
from jax import lax
from jax.experimental import pallas as pl
from jax.experimental.pallas import tpu as pltpu
from jax.sharding import PartitionSpec as P

D = 4096
EPS = 1e-05
ROWS = 128
HALF = 64
DL = 1024
R = 512
STEPS = 3
SEQS = 4
F32 = jnp.float32
BF16 = jnp.bfloat16
MESH = pl.DeviceIdType.MESH

IN_SPLIT = ((0, 1024, "x"),)
OUT_SPLITS = (((0, 768, "x"), (768, 256, "y")), ((0, 768, "x"), (768, 256, "y")))
N_RECV = 87
N_SEND = 18
scope = jax.named_scope


def dot_nt(a, b):
    return lax.dot_general(a, b, (((1,), (1,)), ((), ())), preferred_element_type=F32)


def dot_nn(a, b):
    return lax.dot_general(a, b, (((1,), (0,)), ((), ())), preferred_element_type=F32)


def dot_tn(a, b):
    return lax.dot_general(a, b, (((0,), (0,)), ((), ())), preferred_element_type=F32)


def kernel(
    sections,
    saved_hbm, win_hbm, wout_hbm, gain_hbm, arriving_hbm, logp_hbm, rewards_hbm, lengths_hbm, ids_hbm,
    gin, gout, leaving,
    xs, win, wout, gain, lg, call, gained, hid, gs, coef,
    part_pre, part_back, d_pre, d_back, chip_pre, chip_back, y_pre, y_back,
    sqp, sq, sq_d, sq_chip, sq_y, inv, slope, presum, cout,
    rw, rw_in, weight, rewards, lengths, ids,
    g, h1, f1, s1, h2, f2, gx, gl,
    load_sem, send_sem, recv_sem, shift_send, shift_recv,
):
    sec = lax.axis_index("pipe")
    dp = lax.axis_index("dp")
    tn = lax.axis_index("tensor")
    xi = dp // 4
    yi = dp % 4
    core = tn % 2
    mine = pl.multiple_of(core * HALF, HALF)
    other = pl.multiple_of((1 - core) * HALF, HALF)
    top = sec == sections - 1
    early = [jnp.where(sec == 0, 1 - a, a) for a in range(2)]
    block = [early, [0, 1], [0, 1]]

    partner = (sec, dp, tn + 1 - 2 * core)
    across = (sec, dp, (tn + 2) % 4)
    below = ((sec + sections - 1) % sections, dp, tn)
    above = ((sec + 1) % sections, dp, tn)

    def at_x(to):
        return (sec, to * 4 + yi, tn)

    def at_y(to):
        return (sec, xi * 4 + to, tn)

    def ring(i, by):
        return (i + by) % 4

    peers = [partner, across, below, above]
    peers += [at_x(ring(xi, by)) for by in (1, 2, 3)]
    peers += [at_y(ring(yi, by)) for by in (1, 2, 3)]
    barrier = pltpu.get_barrier_semaphore()
    for peer in peers:
        pl.semaphore_signal(barrier, inc=1, device_id=peer, device_id_type=MESH)

    recv_used = [0]
    classes = {}

    def recv_slot():
        recv_used[0] += 1
        return recv_sem.at[recv_used[0] - 1]

    def send_slot(name, whole):
        if name not in classes:
            classes[name] = (send_sem.at[len(classes)], whole)
        return classes[name][0]

    def remote(src, dst, device, name, whole, recv=None):
        copy = pltpu.make_async_remote_copy(
            src_ref=src, dst_ref=dst, send_sem=send_slot(name, whole),
            recv_sem=recv_slot() if recv is None else recv,
            device_id=device, device_id_type=MESH,
        )
        copy.start()
        return copy

    def arrived(whole, recv):
        pltpu.make_async_remote_copy(
            src_ref=whole, dst_ref=whole, send_sem=send_sem.at[0], recv_sem=recv,
            device_id=partner, device_id_type=MESH,
        ).wait_recv()

    loads = {}

    def load(name, src, dst):
        copy = pltpu.make_async_copy(src, dst, load_sem.at[len(loads)])
        copy.start()
        loads[name] = copy

    load("gain", gain_hbm, gain)
    for a in range(2):
        v = early[a]
        load(("x", 0, a), saved_hbm.at[0, v], xs.at[0, v])
        load(("win", a), win_hbm.at[v], win.at[v])
        load(("c", a), arriving_hbm.at[v], call.at[v, pl.ds(0, ROWS)])
        load(("wout", a), wout_hbm.at[v], wout.at[v])
        if a == 0:
            load("rewards", rewards_hbm, rewards)
            load("lengths", lengths_hbm, lengths)
            load("ids", ids_hbm, ids)
    for t in (2, 1):
        load(("x", t), saved_hbm.at[t], xs.at[t])
    load("lg", logp_hbm, lg)

    rows_of = [pl.ds(t * ROWS, ROWS) for t in range(STEPS)]

    def sixteen(start):
        return pl.ds(pl.multiple_of(start, 16), 16)

    back_copy, pre_copy, sq_copy, hid_copy, gs_copy = {}, {}, {}, {}, {}

    def back_part(t, a):
        v = block[t][a]
        with scope(f"back_part{t}{a}"):
            for n in range(2):
                cols = pl.ds(n * 256, 256)
                part_back[t, a, :, cols] = dot_nt(
                    call[v, rows_of[t], :], wout[v, cols, :]
                ).astype(BF16)

    def back_send(t, a):
        back_copy[t, a] = remote(
            part_back.at[t, a, pl.ds(other, HALF)], d_back.at[t, a], partner, "back", d_back
        )

    def pre_part(t, a):
        v = block[t][a]
        with scope(f"pre_part{t}{a}"):
            gain_row = gain[v]

            def body(i, carry):
                values = xs[t, v, sixteen(i * 16), :].astype(F32)
                gained[v, sixteen(t * ROWS + i * 16), :] = (values * gain_row).astype(BF16)
                squares = values * values
                part = squares[:, 0:128]
                for k in range(1, DL // 128):
                    part = part + squares[:, k * 128 : (k + 1) * 128]
                sqp[sixteen(i * 16), :] = part
                return carry

            lax.fori_loop(0, ROWS // 16, body, 0, unroll=2)
            for n in range(2):
                cols = pl.ds(n * 256, 256)
                part_pre[t, a, :, cols] = dot_nt(
                    gained[v, rows_of[t], :], win[v, cols, :]
                ).astype(BF16)
            total = jnp.sum(sqp[...], axis=-1, keepdims=True)
            same = lax.broadcasted_iota(jnp.int32, (ROWS, 128), 0) == lax.broadcasted_iota(
                jnp.int32, (ROWS, 128), 1
            )
            row = jnp.sum(jnp.where(same, total, 0.0), axis=0, keepdims=True)
            sq[t, a] = jnp.broadcast_to(row, (8, 128))

    def pre_send(t, a):
        pre_copy[t, a] = remote(
            part_pre.at[t, a, pl.ds(other, HALF)], d_pre.at[t, a], partner, "pre", d_pre
        )
        sq_copy[t, a] = remote(sq.at[t, a], sq_d.at[t, a], partner, "sq", sq_d)

    def chip_sum(t, a, copy, part, came, chip, far, name):
        copy.wait_recv()
        chip[t, a] = (
            part[t, a, pl.ds(mine, HALF), :].astype(F32) + came[t, a].astype(F32)
        ).astype(BF16)
        return remote(chip.at[t, a], far.at[t, a], across, name, far)

    def back_chip(t, a):
        with scope(f"back_chip{t}{a}"):
            back_copy[t, a] = chip_sum(
                t, a, back_copy[t, a], part_back, d_back, chip_back, y_back, "far_back"
            )

    def pre_chip(t, a):
        with scope(f"pre_chip{t}{a}"):
            pre_copy[t, a] = chip_sum(
                t, a, pre_copy[t, a], part_pre, d_pre, chip_pre, y_pre, "far_pre"
            )
            sq_copy[t, a].wait_recv()
            sq_chip[t, a] = sq[t, a] + sq_d[t, a]
            sq_copy[t, a] = remote(sq_chip.at[t, a], sq_y.at[t, a], across, "far_sq", sq_y)

    def hidden_of(t, a):
        v = block[t][a]
        with scope(f"hid_wait{t}{a}"):
            sq_copy[t, a].wait_recv()
            pre_copy[t, a].wait_recv()
        with scope(f"hidden{t}{a}"):
            total = sq_chip[t, a] + sq_y[t, a]
            inv_row = (1.0 / jnp.sqrt(total / D + EPS))[0:1, :]
            lane = lax.broadcasted_iota(jnp.int32, (HALF, 128), 1)
            line = lax.broadcasted_iota(jnp.int32, (HALF, 128), 0)
            scale = jnp.sum(jnp.where(lane == line + mine, inv_row, 0.0), axis=-1, keepdims=True)
            inv[t, a] = jnp.broadcast_to(scale, (HALF, 128))

            def body(i, carry):
                r = sixteen(i * 16)
                total = chip_pre[t, a, r, :].astype(F32) + y_pre[t, a, r, :].astype(F32)
                pre = inv[t, a, r, 0:1] * total
                sigma = jax.nn.sigmoid(pre)
                presum[t, a, r, :] = total
                slope[t, a, r, :] = sigma * (1.0 + pre * (1.0 - sigma))
                hid[v, sixteen(t * ROWS + mine + i * 16), :] = (pre * sigma).astype(BF16)
                return carry

            lax.fori_loop(0, HALF // 16, body, 0, unroll=True)
            own = pl.ds(pl.multiple_of(t * ROWS + mine, HALF), HALF)
            hid_copy[t, a] = remote(hid.at[v, own], hid.at[v, own], partner, "hid", d_pre)

    def scaled_of(t, a):
        v = block[t][a]
        with scope(f"gs_wait{t}{a}"):
            back_copy[t, a].wait_recv()
        with scope(f"scaled{t}{a}"):

            def body(i, carry):
                r = sixteen(i * 16)
                back = chip_back[t, a, r, :].astype(F32) + y_back[t, a, r, :].astype(F32)
                scale = inv[t, a, r, 0:1]
                grad_pre = back * slope[t, a, r, :]
                gs[v, sixteen(t * ROWS + mine + i * 16), :] = (scale * grad_pre).astype(BF16)
                radial = jnp.sum(grad_pre * presum[t, a, r, :], axis=-1, keepdims=True)
                amount = scale * scale * scale * radial / D
                coef[t, a, sixteen(mine + i * 16), :] = jnp.broadcast_to(amount, (16, 128))
                return carry

            lax.fori_loop(0, HALF // 16, body, 0, unroll=True)
            own = pl.ds(pl.multiple_of(t * ROWS + mine, HALF), HALF)
            here = pl.ds(mine, HALF)
            gs_copy[t, a] = (
                remote(gs.at[v, own], gs.at[v, own], partner, "gs", d_pre),
                remote(
                    coef.at[t, a, here], coef.at[t, a, here], partner, "coef",
                    coef.at[:, :, pl.ds(0, HALF)],
                ),
            )

    def gs_wait(t, a):
        with scope(f"gs_come{t}{a}"):
            for copy in gs_copy[t, a]:
                copy.wait_recv()

    def cot_out(t, a):
        v = block[t][a]
        with scope(f"cot_out{t}{a}"):
            amount = coef[t, a]
            for n in range(4):
                cols = pl.ds(n * 256, 256)
                product = dot_nn(gs[v, rows_of[t], :], win[v, :, cols])
                out = (
                    call[v, rows_of[t], cols].astype(F32)
                    + gain[v, :, cols] * product
                    - xs[t, v, :, cols].astype(F32) * amount[:, :1]
                ).astype(BF16)
                if t < STEPS - 1:
                    cout[t, a, :, cols] = out
                else:
                    leaving[v, :, cols] = out

    def shift_copy(t, a):
        slot = a if t == 0 or a == 0 else jnp.where(sec == 0, 0, 1)
        return pltpu.make_async_remote_copy(
            src_ref=cout.at[t, a], dst_ref=call.at[slot, rows_of[t + 1]],
            send_sem=shift_send.at[t * 2 + a], recv_sem=shift_recv.at[t * 2 + slot],
            device_id=below, device_id_type=MESH,
        )

    def shift_do(t, a, what):
        if a == t:
            what(shift_copy(t, a))
        else:
            @pl.when(sec != 0)
            def _():
                what(shift_copy(t, a))

    def shift(t, a):
        shift_do(t, a, lambda copy: copy.start())

    def shift_in(t, a):
        v = block[t][a]
        with scope(f"shift_in{t}{a}"):

            @pl.when(jnp.logical_not(jnp.logical_and(top, v == 1)))
            def _():
                arrived(call.at[v, rows_of[t]], shift_recv.at[(t - 1) * 2 + v])

    class Ring:
        def __init__(self, p, out, v, direct, first, width, axis):
            self.direct = direct
            self.p, self.out, self.v = p, out, v
            self.first, self.width = first, width
            self.name = f"{p}{axis}"
            cols = self.cols = pl.ds(first, width)
            pair = ((xi, at_x), (yi, at_y))
            if axis == "x":
                self.axes = pair
                chunk = lambda j, lo, n: g.at[p, j, pl.ds(lo, n), :, cols]
            else:
                self.axes = pair[::-1]
                chunk = lambda j, lo, n: g.at[p, pl.ds(lo, n), j, :, cols]
            small = lambda j, lo, n: s1.at[p, j, pl.ds(lo, n), cols]
            self.chunk = (chunk, small)
            self.n = (2, 16)
            self.half = (h1.at[p, :, :, :, cols], h2.at[p, :, :, cols])
            self.full = (f1.at[p, :, :, :, cols], f2.at[p, pl.ds(0, 3 if direct else 2), :, cols])
            self.half_recv = [recv_slot() for _ in range(1 if direct else 2)]
            self.full_recv = [recv_slot() for _ in range(2)]

        def go(self, phase, j, lo, d, full):
            i, at = self.axes[phase]
            n = self.n[phase]
            src = self.chunk[phase](j, lo, n)
            to = at(ring(i, (1, 3)[d]))
            if full:
                dst = self.full[phase].at[d, pl.ds(lo, n)]
                whole = (f1, f2.at[pl.ds(0, 2), pl.ds(0, 2)])[phase]
                remote(src, dst, to, f"f{phase}", whole, self.full_recv[phase])
            else:
                dst = self.half[phase].at[d]
                whole = (h1, h2.at[pl.ds(0, 2)])[phase]
                remote(src, dst, to, f"h{phase}", whole, self.half_recv[phase])

        def h(self, phase):
            far, n = ring(self.axes[phase][0], 2), self.n[phase]
            self.go(phase, far, 0, 0, False)
            self.go(phase, far, n, 1, False)

        def f(self, phase):
            i, n = self.axes[phase][0], self.n[phase]
            self.go(phase, ring(i, 1), n, 0, True)
            self.go(phase, ring(i, 3), 0, 1, True)

        def m(self, phase):
            i, n = self.axes[phase][0], self.n[phase]
            with scope(f"m{phase}_{self.name}"):
                arrived(self.half[phase], self.half_recv[phase])
                for d, j, lo in ((0, ring(i, 1), 0), (1, ring(i, 3), n)):
                    chunk = self.chunk[phase](j, lo, n)
                    came = self.half[phase].at[d]
                    chunk[...] = (chunk[...].astype(F32) + came[...].astype(F32)).astype(BF16)
                    self.go(phase, j, lo, d, True)

        def second(self):
            if not self.direct:
                self.h(1)
                self.f(1)
                return
            i, at = self.axes[1]
            for k, by in enumerate((2, 1, 3)):
                j = ring(i, by)
                remote(
                    self.chunk[1](j, 0, 32), self.full[1].at[k], at(j), "direct",
                    f2.at[pl.ds(0, 2)], self.full_recv[1],
                )

        def middle(self):
            with scope(f"mid_{self.name}"):
                arrived(self.full[0], self.full_recv[0])
                i = self.axes[0][0]
                for k in range(4):
                    total = self.chunk[0](i, k, 1)[...].reshape(32, self.width).astype(F32)
                    for d in range(2):
                        total = total + f1[self.p, d, k, :, self.cols].astype(F32)
                    s1[self.p, k, :, self.cols] = total.astype(BF16)
                self.second()

        def end(self):
            with scope(f"end_{self.name}"):
                arrived(self.full[1], self.full_recv[1])
                total = s1[self.p, self.axes[1][0], :, self.cols].astype(F32)
                for d in range(3 if self.direct else 2):
                    total = total + f2[self.p, d, :, self.cols].astype(F32)
                self.out[self.v, :, self.cols] = total * (1.0 / (16 * ROWS))

    def grad(p, left, right, v, steps):
        with scope(f"grad_{p}"):
            tokens = pl.ds(0, steps * ROWS)
            lhs = left[v, tokens, :]
            for k in (3, 0, 1, 2):
                cols = pl.ds(k * 256, 256)
                made = dot_tn(lhs, right[v, tokens, cols]).astype(BF16)
                g[p, :, :, :, cols] = made.reshape(4, 4, 32, 256)

    gx_recv = [[recv_slot() for _ in range(3)] for _ in range(2)]
    gl_recv = [recv_slot() for _ in range(2)]
    nxt, prv, far = (at_x(ring(xi, by)) for by in (1, 3, 2))

    def slot_rows(k, lo=0, n=ROWS):
        return pl.ds(k * ROWS + lo, n)

    def gather(v):
        own = gained.at[v, rows_of[2]]
        remote(own, gx.at[v, slot_rows(0)], nxt, "gx", gx.at[:, pl.ds(0, 2 * ROWS)], gx_recv[v][0])
        remote(own, gx.at[v, slot_rows(1)], prv, "gx", None, gx_recv[v][1])

    def forward(v):
        with scope(f"forward{v}"):
            for k, lo, to in ((0, 0, nxt), (1, HALF, prv)):
                arrived(gx.at[v, slot_rows(k)], gx_recv[v][k])
                remote(
                    gx.at[v, slot_rows(k, lo, HALF)], gx.at[v, slot_rows(2, lo, HALF)], to, "gx2",
                    gx.at[:, pl.ds(0, ROWS)], gx_recv[v][2],
                )

    def left_send(v):
        for k, by, to in ((0, 1, nxt), (1, 3, prv), (2, 2, far)):
            cols = pl.ds(pl.multiple_of(ring(xi, by) * 128, 128), 128)
            remote(gs.at[v, rows_of[2], cols], gl.at[v, slot_rows(k)], to, "gl", gl, gl_recv[v])

    def in_middle(ring_):
        v, p = ring_.v, ring_.p
        with scope(f"mid_{ring_.name}"):
            arrived(ring_.full[0], ring_.full_recv[0])
            arrived(gx.at[v, slot_rows(2)], gx_recv[v][2])
            arrived(gl.at[v], gl_recv[v])
            own = gs[v, rows_of[2], pl.ds(pl.multiple_of(xi * 128, 128), 128)]
            for k in range(4):
                cols = pl.ds(k * 256, 256)
                total = dot_tn(gl[v], gx[v, :, cols]) + dot_tn(own, gained[v, rows_of[2], cols])
                total = total + g[p, xi, :, :, cols].reshape(128, 256).astype(F32)
                for d in range(2):
                    total = total + f1[p, d, :, :, cols].reshape(128, 256).astype(F32)
                s1[p, :, :, cols] = total.astype(BF16).reshape(4, 32, 256)
            ring_.second()

    loads["gain"].wait()
    for a in range(2):
        loads[("x", 0, a)].wait()
        loads[("win", a)].wait()
        pre_part(0, a)
        loads[("c", a)].wait()
        loads[("wout", a)].wait()
        back_part(0, a)
    for name in ("rewards", "lengths", "ids"):
        loads[name].wait()
    lane = lax.broadcasted_iota(jnp.int32, (8, 128), 1)
    line = lax.broadcasted_iota(jnp.int32, (8, 128), 0)
    tile = jnp.zeros((8, 128), F32)
    for n in range(2):
        for k in range(SEQS):
            member = lane == ids[n, 0, k]
            amount = jnp.where(line == 0, rewards[n, 0, k], jnp.where(line == 1, 1.0, 0.0))
            tile = tile + jnp.where(member, amount, 0.0)
    rw[0] = tile
    with scope("barrier"):
        pl.semaphore_wait(barrier, len(peers))
    for a in range(2):
        pre_send(0, a)
        back_send(0, a)
    rw_x = [
        remote(rw.at[0], rw_in.at[k], to, "rw", rw_in) for k, to in ((0, nxt), (1, prv), (2, far))
    ]
    rw_y = [at_y(yi + 1 - 2 * (yi % 2)), at_y(3 - yi)]

    def rw_send(k):
        return remote(rw.at[k], rw_in.at[k + 2], rw_y[k - 1], "rw", rw_in)

    def rw_add(k, copy):
        with scope(f"rw{k}"):
            copy.wait_recv()
            rw[k + 1] = rw[k] + rw_in[k + 2]

    loads[("x", 2)].wait()
    pre_part(2, 0)
    gather(0)
    pre_chip(0, 0)
    back_chip(0, 0)
    pre_send(2, 0)
    pre_part(2, 1)
    gather(1)
    pre_send(2, 1)
    loads[("x", 1)].wait()
    pre_part(1, 0)
    pre_send(1, 0)
    pre_chip(0, 1)
    back_chip(0, 1)
    pre_part(1, 1)
    pre_send(1, 1)
    hidden_of(0, 0)
    scaled_of(0, 0)
    with scope("rwx"):
        for copy in rw_x:
            copy.wait_recv()
        rw[1] = rw[0] + rw_in[0] + rw_in[1] + rw_in[2]
    rw_copy = rw_send(1)
    gs_wait(0, 0)
    cot_out(0, 0)
    shift(0, 0)
    hidden_of(0, 1)
    pre_chip(1, 0)
    scaled_of(0, 1)
    gs_wait(0, 1)
    cot_out(0, 1)
    shift(0, 1)

    rw_add(1, rw_copy)
    rw_copy = rw_send(2)
    pre_chip(1, 1)
    pre_chip(2, 0)
    pre_chip(2, 1)
    forward(0)
    hidden_of(1, 0)

    shift_in(1, 0)
    back_part(1, 0)
    back_send(1, 0)
    hidden_of(1, 1)
    back_chip(1, 0)
    forward(1)
    rw_add(2, rw_copy)
    loads["lg"].wait()
    with scope("entering"):

        @pl.when(top)
        def _():
            sums = rw[3]
            means = sums[0:1, :] / jnp.maximum(sums[1:2, :], 1.0)
            position = lax.broadcasted_iota(jnp.int32, (ROWS, 128), 0)
            for n in range(2):
                begin = jnp.int32(0)
                weights = jnp.zeros((ROWS, 128), F32)
                for k in range(SEQS):
                    finish = begin + lengths[n, 0, k]
                    own = jnp.sum(
                        jnp.where(lane[0:1, :] == ids[n, 0, k], means, 0.0), axis=-1, keepdims=True
                    )
                    advantage = rewards[n, 0, k] - own
                    inside = jnp.logical_and(position >= begin, position < finish)
                    weights = weights + jnp.where(inside, advantage, 0.0)
                    begin = finish
                weight[n] = -weights

                def body(i, carry):
                    r = sixteen(i * 16)
                    values = weight[n, r, 0:1] * lg[n, r, :].astype(F32)
                    call[1, sixteen((n + 1) * ROWS + i * 16), :] = values.astype(BF16)
                    return carry

                lax.fori_loop(0, ROWS // 16, body, 0)

    hidden_of(2, 0)
    scaled_of(1, 0)
    shift_in(1, 1)
    back_part(1, 1)
    back_send(1, 1)
    gs_wait(1, 0)
    cot_out(1, 0)
    shift(1, 0)

    out0x, out0y = (Ring(0, gout, 0, True, *split) for split in OUT_SPLITS[0])
    out1x, out1y = (Ring(2, gout, 1, True, *split) for split in OUT_SPLITS[1])
    in0, in1 = (Ring(1 + 2 * v, gin, v, False, *IN_SPLIT[0]) for v in range(2))
    hidden_of(2, 1)
    back_chip(1, 1)
    grad(1, gs, gained, 0, 2)
    in0.h(0)
    in0.f(0)
    for t in range(STEPS):
        for a in range(2):
            hid_copy[t, a].wait_recv()
    scaled_of(1, 1)
    gs_wait(1, 1)
    cot_out(1, 1)
    shift(1, 1)
    grad(3, gs, gained, 1, 2)
    in1.h(0)

    shift_in(2, 0)
    back_part(2, 0)
    back_send(2, 0)
    in0.m(0)
    grad(0, hid, call, 0, 3)
    back_chip(2, 0)
    out0x.h(0)
    out0x.f(0)
    scaled_of(2, 0)
    gs_wait(2, 0)
    left_send(0)
    out0y.h(0)
    shift_in(2, 1)
    back_part(2, 1)
    back_send(2, 1)
    grad(2, hid, call, 1, 3)
    back_chip(2, 1)
    out0x.m(0)
    in1.m(0)
    in1.f(0)
    cot_out(2, 0)
    out0y.m(0)
    out0y.f(0)
    in_middle(in0)
    scaled_of(2, 1)
    gs_wait(2, 1)
    left_send(1)
    out1x.h(0)
    out1y.h(0)
    out0x.middle()
    cot_out(2, 1)
    out1x.f(0)
    out0y.middle()
    in0.m(1)
    out1x.m(0)
    out1y.m(0)
    out1y.f(0)
    in_middle(in1)
    out0x.end()
    in0.end()
    out0y.end()
    out1y.middle()
    out1x.middle()
    in1.m(1)
    in1.end()
    out1y.end()
    out1x.end()

    with scope("ends"):
        for sem, whole in classes.values():
            pltpu.make_async_remote_copy(
                src_ref=whole, dst_ref=whole, send_sem=sem, recv_sem=recv_sem.at[0],
                device_id=partner, device_id_type=MESH,
            ).wait_send()

        for t in range(STEPS - 1):
            for a in range(2):
                shift_do(t, a, lambda copy: copy.wait_send())
    assert (recv_used[0], len(classes), len(loads)) == (N_RECV, N_SEND, 15), (recv_used[0], len(classes), len(loads))


def finish(gin, gout, leaving, gin_hbm, gout_hbm, leaving_hbm, sem):
    pairs = ((leaving, leaving_hbm), (gin, gin_hbm), (gout, gout_hbm))
    copies = [pltpu.make_async_copy(src, dst, sem.at[k]) for k, (src, dst) in enumerate(pairs)]
    for copy in copies:
        copy.start()
    for copy in copies:
        copy.wait()


def shards(saved, proj_in, proj_out, gain, arriving, logp, rewards, lengths, ids):
    sections = lax.axis_size("pipe")
    hbm = pl.BlockSpec(memory_space=pltpu.HBM)
    vmem = pl.BlockSpec(memory_space=pltpu.VMEM)
    V = pltpu.VMEM
    shapes = (
        jax.ShapeDtypeStruct((2, 32, DL), F32),
        jax.ShapeDtypeStruct((2, 32, DL), F32),
        jax.ShapeDtypeStruct((2, ROWS, DL), BF16),
    )
    results = pl.pallas_call(
        lambda *refs: kernel(sections, *refs),
        name="window",
        out_shape=shapes,
        in_specs=[hbm] * 9,
        out_specs=(vmem, vmem, vmem),
        scratch_shapes=[
            V((STEPS, 2, ROWS, DL), BF16),
            V((2, R, DL), BF16),
            V((2, R, DL), BF16),
            V((2, 1, DL), F32),
            V((2, ROWS, DL), BF16),
            V((2, STEPS * ROWS, DL), BF16),
            V((2, STEPS * ROWS, DL), BF16),
            V((2, STEPS * ROWS, R), BF16),
            V((2, STEPS * ROWS, R), BF16),
            V((STEPS, 2, ROWS, 128), F32),
            V((STEPS, 2, ROWS, R), BF16),
            V((STEPS, 2, ROWS, R), BF16),
            V((STEPS, 2, HALF, R), BF16),
            V((STEPS, 2, HALF, R), BF16),
            V((STEPS, 2, HALF, R), BF16),
            V((STEPS, 2, HALF, R), BF16),
            V((STEPS, 2, HALF, R), BF16),
            V((STEPS, 2, HALF, R), BF16),
            V((ROWS, 128), F32),
            V((STEPS, 2, 8, 128), F32),
            V((STEPS, 2, 8, 128), F32),
            V((STEPS, 2, 8, 128), F32),
            V((STEPS, 2, 8, 128), F32),
            V((STEPS, 2, HALF, 128), F32),
            V((STEPS, 2, HALF, R), F32),
            V((STEPS, 2, HALF, R), F32),
            V((STEPS - 1, 2, ROWS, DL), BF16),
            V((4, 8, 128), F32),
            V((5, 8, 128), F32),
            V((2, ROWS, 128), F32),
            pltpu.SMEM((2, 1, SEQS), F32),
            pltpu.SMEM((2, 1, SEQS), jnp.int32),
            pltpu.SMEM((2, 1, SEQS), jnp.int32),
            V((4, 4, 4, 32, DL), BF16),
            V((4, 2, 2, 32, DL), BF16),
            V((4, 2, 4, 32, DL), BF16),
            V((4, 4, 32, DL), BF16),
            V((4, 2, 16, DL), BF16),
            V((4, 3, 32, DL), BF16),
            V((2, 3 * ROWS, DL), BF16),
            V((2, 3 * ROWS, 128), BF16),
            pltpu.SemaphoreType.DMA((15,)),
            pltpu.SemaphoreType.DMA((N_SEND,)),
            pltpu.SemaphoreType.DMA((N_RECV,)),
            pltpu.SemaphoreType.DMA((4,)),
            pltpu.SemaphoreType.DMA((4,)),
        ],
        compiler_params=pltpu.CompilerParams(
            collective_id=0, has_side_effects=True, vmem_limit_bytes=40 * 2**20
        ),
    )(
        *(
            pltpu.with_memory_space_constraint(x, pltpu.HBM)
            for x in (
                saved[:, :, 0], proj_in[:, 0], proj_out[:, 0], gain, arriving[:, 0], logp,
                rewards, lengths, ids,
            )
        )
    )
    any_spec = pl.BlockSpec(memory_space=pl.ANY)
    results = pl.pallas_call(
        finish,
        name="finish",
        out_shape=shapes,
        in_specs=[vmem] * 3,
        out_specs=(any_spec,) * 3,
        scratch_shapes=[pltpu.SemaphoreType.DMA((3,))],
        compiler_params=pltpu.CompilerParams(vmem_limit_bytes=2**20),
    )(*results)
    return tuple(r[:, None] for r in results)


def solution(mesh):
    return jax.shard_map(
        shards,
        mesh=mesh,
        in_specs=(
            P(None, None, "pipe", "dp", "tensor"),
            P(None, "pipe", None, "tensor"),
            P(None, "pipe", None, "tensor"),
            P(None, "pipe", "tensor"),
            P(None, "pipe", "dp", "tensor"),
            P(None, "dp", "tensor"),
            P(None, "dp", None),
            P(None, "dp", None),
            P(None, "dp", None),
        ),
        out_specs=(
            P(None, "pipe", "dp", "tensor"),
            P(None, "pipe", "dp", "tensor"),
            P(None, "pipe", "dp", "tensor"),
        ),
        check_vma=False,
    )
```

```python
import jax
import jax.numpy as jnp
from jax import lax
from jax.experimental import pallas as pl
from jax.experimental.pallas import tpu as pltpu
from jax.sharding import PartitionSpec as P

D = 4096
EPS = 1e-05
ROWS = 128
HALF = 64
DL = 1024
R = 512
STEPS = 3
SEQS = 4
F32 = jnp.float32
BF16 = jnp.bfloat16
MESH = pl.DeviceIdType.MESH

IN_SPLIT = ((0, 1024, "x"),)
OUT_SPLITS = (
    ((0, 768, "x"), (768, 256, "y")),
    ((0, 384, "x"), (384, 384, "x"), (768, 256, "y")),
)
N_RECV = 90
N_SEND = 18
scope = jax.named_scope


def dot_nt(a, b):
    return lax.dot_general(a, b, (((1,), (1,)), ((), ())), preferred_element_type=F32)


def dot_nn(a, b):
    return lax.dot_general(a, b, (((1,), (0,)), ((), ())), preferred_element_type=F32)


def dot_tn(a, b):
    return lax.dot_general(a, b, (((0,), (0,)), ((), ())), preferred_element_type=F32)


def kernel(
    sections,
    saved_hbm, win_hbm, wout_hbm, gain_hbm, arriving_hbm, logp_hbm, rewards_hbm, lengths_hbm, ids_hbm,
    gin, gout, leaving,
    xs, win, wout, gain, lg, call, gained, hid, gs, coef,
    part_pre, part_back, d_pre, d_back, chip_pre, chip_back, y_pre, y_back,
    sqp, sq, sq_d, sq_chip, sq_y, inv, slope, presum, cout,
    rw, rw_in, weight, rewards, lengths, ids,
    g, h1, f1, s1, h2, f2, gx, gl,
    load_sem, send_sem, recv_sem, shift_send, shift_recv,
):
    sec = lax.axis_index("pipe")
    dp = lax.axis_index("dp")
    tn = lax.axis_index("tensor")
    xi = dp // 4
    yi = dp % 4
    core = tn % 2
    mine = pl.multiple_of(core * HALF, HALF)
    other = pl.multiple_of((1 - core) * HALF, HALF)
    top = sec == sections - 1
    early = [jnp.where(sec == 0, 1 - a, a) for a in range(2)]
    block = [early, [0, 1], [0, 1]]

    partner = (sec, dp, tn + 1 - 2 * core)
    across = (sec, dp, (tn + 2) % 4)
    below = ((sec + sections - 1) % sections, dp, tn)
    above = ((sec + 1) % sections, dp, tn)

    def at_x(to):
        return (sec, to * 4 + yi, tn)

    def at_y(to):
        return (sec, xi * 4 + to, tn)

    def ring(i, by):
        return (i + by) % 4

    peers = [partner, across, below, above]
    peers += [at_x(ring(xi, by)) for by in (1, 2, 3)]
    peers += [at_y(ring(yi, by)) for by in (1, 2, 3)]
    barrier = pltpu.get_barrier_semaphore()
    for peer in peers:
        pl.semaphore_signal(barrier, inc=1, device_id=peer, device_id_type=MESH)

    recv_used = [0]
    classes = {}

    def recv_slot():
        recv_used[0] += 1
        return recv_sem.at[recv_used[0] - 1]

    def send_slot(name, whole):
        if name not in classes:
            classes[name] = (send_sem.at[len(classes)], whole)
        return classes[name][0]

    def remote(src, dst, device, name, whole, recv=None):
        copy = pltpu.make_async_remote_copy(
            src_ref=src, dst_ref=dst, send_sem=send_slot(name, whole),
            recv_sem=recv_slot() if recv is None else recv,
            device_id=device, device_id_type=MESH,
        )
        copy.start()
        return copy

    def arrived(whole, recv):
        pltpu.make_async_remote_copy(
            src_ref=whole, dst_ref=whole, send_sem=send_sem.at[0], recv_sem=recv,
            device_id=partner, device_id_type=MESH,
        ).wait_recv()

    loads = {}

    def load(name, src, dst):
        copy = pltpu.make_async_copy(src, dst, load_sem.at[len(loads)])
        copy.start()
        loads[name] = copy

    def load_block(a):
        v = early[a]
        load(("x", 0, a), saved_hbm.at[0, v], xs.at[0, v])
        load(("win", a), win_hbm.at[v], win.at[v])
        load(("c", a), arriving_hbm.at[v], call.at[v, pl.ds(0, ROWS)])
        load(("wout", a), wout_hbm.at[v], wout.at[v])

    load("gain", gain_hbm, gain)
    load_block(0)

    def load_rest():
        load_block(1)
        load("rewards", rewards_hbm, rewards)
        load("lengths", lengths_hbm, lengths)
        load("ids", ids_hbm, ids)
        for t in (2, 1):
            load(("x", t), saved_hbm.at[t], xs.at[t])
        load("lg", logp_hbm, lg)

    rows_of = [pl.ds(t * ROWS, ROWS) for t in range(STEPS)]

    def sixteen(start):
        return pl.ds(pl.multiple_of(start, 16), 16)

    back_copy, pre_copy, sq_copy, hid_copy, gs_copy = {}, {}, {}, {}, {}

    def back_part(t, a):
        v = block[t][a]
        with scope(f"back_part{t}{a}"):
            for n in range(2):
                cols = pl.ds(n * 256, 256)
                part_back[t, a, :, cols] = dot_nt(
                    call[v, rows_of[t], :], wout[v, cols, :]
                ).astype(BF16)

    def back_send(t, a):
        back_copy[t, a] = remote(
            part_back.at[t, a, pl.ds(other, HALF)], d_back.at[t, a], partner, "back", d_back
        )

    def pre_part(t, a):
        v = block[t][a]
        with scope(f"pre_part{t}{a}"):
            gain_row = gain[v]

            def body(i, carry):
                values = xs[t, v, sixteen(i * 16), :].astype(F32)
                gained[v, sixteen(t * ROWS + i * 16), :] = (values * gain_row).astype(BF16)
                squares = values * values
                part = squares[:, 0:128]
                for k in range(1, DL // 128):
                    part = part + squares[:, k * 128 : (k + 1) * 128]
                sqp[sixteen(i * 16), :] = part
                return carry

            lax.fori_loop(0, ROWS // 16, body, 0, unroll=2)
            for n in range(2):
                cols = pl.ds(n * 256, 256)
                part_pre[t, a, :, cols] = dot_nt(
                    gained[v, rows_of[t], :], win[v, cols, :]
                ).astype(BF16)
            total = jnp.sum(sqp[...], axis=-1, keepdims=True)
            same = lax.broadcasted_iota(jnp.int32, (ROWS, 128), 0) == lax.broadcasted_iota(
                jnp.int32, (ROWS, 128), 1
            )
            row = jnp.sum(jnp.where(same, total, 0.0), axis=0, keepdims=True)
            sq[t, a] = jnp.broadcast_to(row, (8, 128))

    def pre_send(t, a):
        pre_copy[t, a] = remote(
            part_pre.at[t, a, pl.ds(other, HALF)], d_pre.at[t, a], partner, "pre", d_pre
        )
        sq_copy[t, a] = remote(sq.at[t, a], sq_d.at[t, a], partner, "sq", sq_d)

    def chip_sum(t, a, copy, part, came, chip, far, name):
        copy.wait_recv()
        chip[t, a] = (
            part[t, a, pl.ds(mine, HALF), :].astype(F32) + came[t, a].astype(F32)
        ).astype(BF16)
        return remote(chip.at[t, a], far.at[t, a], across, name, far)

    def back_chip(t, a):
        with scope(f"back_chip{t}{a}"):
            back_copy[t, a] = chip_sum(
                t, a, back_copy[t, a], part_back, d_back, chip_back, y_back, "far_back"
            )

    def pre_chip(t, a):
        with scope(f"pre_chip{t}{a}"):
            pre_copy[t, a] = chip_sum(
                t, a, pre_copy[t, a], part_pre, d_pre, chip_pre, y_pre, "far_pre"
            )
            sq_copy[t, a].wait_recv()
            sq_chip[t, a] = sq[t, a] + sq_d[t, a]
            sq_copy[t, a] = remote(sq_chip.at[t, a], sq_y.at[t, a], across, "far_sq", sq_y)

    def hidden_of(t, a):
        v = block[t][a]
        with scope(f"hid_wait{t}{a}"):
            sq_copy[t, a].wait_recv()
            pre_copy[t, a].wait_recv()
        with scope(f"hidden{t}{a}"):
            total = sq_chip[t, a] + sq_y[t, a]
            inv_row = (1.0 / jnp.sqrt(total / D + EPS))[0:1, :]
            lane = lax.broadcasted_iota(jnp.int32, (HALF, 128), 1)
            line = lax.broadcasted_iota(jnp.int32, (HALF, 128), 0)
            scale = jnp.sum(jnp.where(lane == line + mine, inv_row, 0.0), axis=-1, keepdims=True)
            inv[t, a] = jnp.broadcast_to(scale, (HALF, 128))

            def body(i, carry):
                r = sixteen(i * 16)
                total = chip_pre[t, a, r, :].astype(F32) + y_pre[t, a, r, :].astype(F32)
                pre = inv[t, a, r, 0:1] * total
                sigma = jax.nn.sigmoid(pre)
                presum[t, a, r, :] = total
                slope[t, a, r, :] = sigma * (1.0 + pre * (1.0 - sigma))
                hid[v, sixteen(t * ROWS + mine + i * 16), :] = (pre * sigma).astype(BF16)
                return carry

            lax.fori_loop(0, HALF // 16, body, 0, unroll=True)
            own = pl.ds(pl.multiple_of(t * ROWS + mine, HALF), HALF)
            hid_copy[t, a] = remote(hid.at[v, own], hid.at[v, own], partner, "hid", d_pre)

    def scaled_of(t, a):
        v = block[t][a]
        with scope(f"gs_wait{t}{a}"):
            back_copy[t, a].wait_recv()
        with scope(f"scaled{t}{a}"):

            def body(i, carry):
                r = sixteen(i * 16)
                back = chip_back[t, a, r, :].astype(F32) + y_back[t, a, r, :].astype(F32)
                scale = inv[t, a, r, 0:1]
                grad_pre = back * slope[t, a, r, :]
                gs[v, sixteen(t * ROWS + mine + i * 16), :] = (scale * grad_pre).astype(BF16)
                radial = jnp.sum(grad_pre * presum[t, a, r, :], axis=-1, keepdims=True)
                amount = scale * scale * scale * radial / D
                coef[t, a, sixteen(mine + i * 16), :] = jnp.broadcast_to(amount, (16, 128))
                return carry

            lax.fori_loop(0, HALF // 16, body, 0, unroll=True)
            own = pl.ds(pl.multiple_of(t * ROWS + mine, HALF), HALF)
            here = pl.ds(mine, HALF)
            gs_copy[t, a] = (
                remote(gs.at[v, own], gs.at[v, own], partner, "gs", d_pre),
                remote(
                    coef.at[t, a, here], coef.at[t, a, here], partner, "coef",
                    coef.at[:, :, pl.ds(0, HALF)],
                ),
            )

    def gs_wait(t, a):
        with scope(f"gs_come{t}{a}"):
            for copy in gs_copy[t, a]:
                copy.wait_recv()

    def cot_out(t, a):
        v = block[t][a]
        with scope(f"cot_out{t}{a}"):
            amount = coef[t, a]
            for n in range(4):
                cols = pl.ds(n * 256, 256)
                product = dot_nn(gs[v, rows_of[t], :], win[v, :, cols])
                out = (
                    call[v, rows_of[t], cols].astype(F32)
                    + gain[v, :, cols] * product
                    - xs[t, v, :, cols].astype(F32) * amount[:, :1]
                ).astype(BF16)
                if t < STEPS - 1:
                    cout[t, a, :, cols] = out
                else:
                    leaving[v, :, cols] = out

    def shift_copy(t, a):
        slot = a if t == 0 or a == 0 else jnp.where(sec == 0, 0, 1)
        return pltpu.make_async_remote_copy(
            src_ref=cout.at[t, a], dst_ref=call.at[slot, rows_of[t + 1]],
            send_sem=shift_send.at[t * 2 + a], recv_sem=shift_recv.at[t * 2 + slot],
            device_id=below, device_id_type=MESH,
        )

    def shift_do(t, a, what):
        if a == t:
            what(shift_copy(t, a))
        else:
            @pl.when(sec != 0)
            def _():
                what(shift_copy(t, a))

    def shift(t, a):
        shift_do(t, a, lambda copy: copy.start())

    def shift_in(t, a):
        v = block[t][a]
        with scope(f"shift_in{t}{a}"):

            @pl.when(jnp.logical_not(jnp.logical_and(top, v == 1)))
            def _():
                arrived(call.at[v, rows_of[t]], shift_recv.at[(t - 1) * 2 + v])

    class Ring:
        def __init__(self, p, out, v, direct, first, width, axis):
            self.direct = direct
            self.p, self.out, self.v = p, out, v
            self.first, self.width = first, width
            self.name = f"{p}{axis}{first}"
            cols = self.cols = pl.ds(first, width)
            pair = ((xi, at_x), (yi, at_y))
            if axis == "x":
                self.axes = pair
                chunk = lambda j, lo, n: g.at[p, j, pl.ds(lo, n), :, cols]
            else:
                self.axes = pair[::-1]
                chunk = lambda j, lo, n: g.at[p, pl.ds(lo, n), j, :, cols]
            small = lambda j, lo, n: s1.at[p, j, pl.ds(lo, n), cols]
            self.chunk = (chunk, small)
            self.n = (2, 16)
            self.half = (h1.at[p, :, :, :, cols], h2.at[p, :, :, cols])
            self.full = (f1.at[p, :, :, :, cols], f2.at[p, pl.ds(0, 3 if direct else 2), :, cols])
            self.half_recv = [recv_slot() for _ in range(1 if direct else 2)]
            self.full_recv = [recv_slot() for _ in range(2)]

        def go(self, phase, j, lo, d, full):
            i, at = self.axes[phase]
            n = self.n[phase]
            src = self.chunk[phase](j, lo, n)
            to = at(ring(i, (1, 3)[d]))
            if full:
                dst = self.full[phase].at[d, pl.ds(lo, n)]
                whole = (f1, f2.at[pl.ds(0, 2), pl.ds(0, 2)])[phase]
                remote(src, dst, to, f"f{phase}", whole, self.full_recv[phase])
            else:
                dst = self.half[phase].at[d]
                whole = (h1, h2.at[pl.ds(0, 2)])[phase]
                remote(src, dst, to, f"h{phase}", whole, self.half_recv[phase])

        def h(self, phase):
            far, n = ring(self.axes[phase][0], 2), self.n[phase]
            self.go(phase, far, 0, 0, False)
            self.go(phase, far, n, 1, False)

        def f(self, phase):
            i, n = self.axes[phase][0], self.n[phase]
            self.go(phase, ring(i, 1), n, 0, True)
            self.go(phase, ring(i, 3), 0, 1, True)

        def m(self, phase):
            i, n = self.axes[phase][0], self.n[phase]
            with scope(f"m{phase}_{self.name}"):
                arrived(self.half[phase], self.half_recv[phase])
                for d, j, lo in ((0, ring(i, 1), 0), (1, ring(i, 3), n)):
                    chunk = self.chunk[phase](j, lo, n)
                    came = self.half[phase].at[d]
                    chunk[...] = (chunk[...].astype(F32) + came[...].astype(F32)).astype(BF16)
                    self.go(phase, j, lo, d, True)

        def second(self):
            if not self.direct:
                self.h(1)
                self.f(1)
                return
            i, at = self.axes[1]
            for k, by in enumerate((2, 1, 3)):
                j = ring(i, by)
                remote(
                    self.chunk[1](j, 0, 32), self.full[1].at[k], at(j), "direct",
                    f2.at[pl.ds(0, 2)], self.full_recv[1],
                )

        def middle(self):
            with scope(f"mid_{self.name}"):
                arrived(self.full[0], self.full_recv[0])
                i = self.axes[0][0]
                for k in range(4):
                    total = self.chunk[0](i, k, 1)[...].reshape(32, self.width).astype(F32)
                    for d in range(2):
                        total = total + f1[self.p, d, k, :, self.cols].astype(F32)
                    s1[self.p, k, :, self.cols] = total.astype(BF16)
                self.second()

        def end(self):
            with scope(f"end_{self.name}"):
                arrived(self.full[1], self.full_recv[1])
                total = s1[self.p, self.axes[1][0], :, self.cols].astype(F32)
                for d in range(3 if self.direct else 2):
                    total = total + f2[self.p, d, :, self.cols].astype(F32)
                self.out[self.v, :, self.cols] = total * (1.0 / (16 * ROWS))

    def grad(p, left, right, v, steps):
        with scope(f"grad_{p}"):
            tokens = pl.ds(0, steps * ROWS)
            lhs = left[v, tokens, :]
            for k in (3, 0, 1, 2):
                cols = pl.ds(k * 256, 256)
                made = dot_tn(lhs, right[v, tokens, cols]).astype(BF16)
                g[p, :, :, :, cols] = made.reshape(4, 4, 32, 256)

    gx_recv = [[recv_slot() for _ in range(3)] for _ in range(2)]
    gl_recv = [recv_slot() for _ in range(2)]
    nxt, prv, far = (at_x(ring(xi, by)) for by in (1, 3, 2))

    def slot_rows(k, lo=0, n=ROWS):
        return pl.ds(k * ROWS + lo, n)

    def gather(v):
        own = gained.at[v, rows_of[2]]
        remote(own, gx.at[v, slot_rows(0)], nxt, "gx", gx.at[:, pl.ds(0, 2 * ROWS)], gx_recv[v][0])
        remote(own, gx.at[v, slot_rows(1)], prv, "gx", None, gx_recv[v][1])

    def forward(v):
        with scope(f"forward{v}"):
            for k, lo, to in ((0, 0, nxt), (1, HALF, prv)):
                arrived(gx.at[v, slot_rows(k)], gx_recv[v][k])
                remote(
                    gx.at[v, slot_rows(k, lo, HALF)], gx.at[v, slot_rows(2, lo, HALF)], to, "gx2",
                    gx.at[:, pl.ds(0, ROWS)], gx_recv[v][2],
                )

    def left_send(v):
        for k, by, to in ((0, 1, nxt), (1, 3, prv), (2, 2, far)):
            cols = pl.ds(pl.multiple_of(ring(xi, by) * 128, 128), 128)
            remote(gs.at[v, rows_of[2], cols], gl.at[v, slot_rows(k)], to, "gl", gl, gl_recv[v])

    def in_middle(ring_):
        v, p = ring_.v, ring_.p
        with scope(f"mid_{ring_.name}"):
            arrived(ring_.full[0], ring_.full_recv[0])
            arrived(gx.at[v, slot_rows(2)], gx_recv[v][2])
            arrived(gl.at[v], gl_recv[v])
            own = gs[v, rows_of[2], pl.ds(pl.multiple_of(xi * 128, 128), 128)]
            for k in range(4):
                cols = pl.ds(k * 256, 256)
                total = dot_tn(gl[v], gx[v, :, cols]) + dot_tn(own, gained[v, rows_of[2], cols])
                total = total + g[p, xi, :, :, cols].reshape(128, 256).astype(F32)
                for d in range(2):
                    total = total + f1[p, d, :, :, cols].reshape(128, 256).astype(F32)
                s1[p, :, :, cols] = total.astype(BF16).reshape(4, 32, 256)
            ring_.second()

    loads["gain"].wait()
    loads[("x", 0, 0)].wait()
    loads[("win", 0)].wait()
    load_rest()
    pre_part(0, 0)
    loads[("c", 0)].wait()
    loads[("wout", 0)].wait()
    back_part(0, 0)
    with scope("barrier"):
        pl.semaphore_wait(barrier, len(peers))
    pre_send(0, 0)
    back_send(0, 0)
    loads[("x", 0, 1)].wait()
    loads[("win", 1)].wait()
    pre_part(0, 1)
    pre_send(0, 1)
    loads[("c", 1)].wait()
    loads[("wout", 1)].wait()
    back_part(0, 1)
    back_send(0, 1)
    pre_chip(0, 0)
    back_chip(0, 0)
    for name in ("rewards", "lengths", "ids"):
        loads[name].wait()
    lane = lax.broadcasted_iota(jnp.int32, (8, 128), 1)
    line = lax.broadcasted_iota(jnp.int32, (8, 128), 0)
    tile = jnp.zeros((8, 128), F32)
    for n in range(2):
        for k in range(SEQS):
            member = lane == ids[n, 0, k]
            amount = jnp.where(line == 0, rewards[n, 0, k], jnp.where(line == 1, 1.0, 0.0))
            tile = tile + jnp.where(member, amount, 0.0)
    rw[0] = tile
    rw_x = [
        remote(rw.at[0], rw_in.at[k], to, "rw", rw_in) for k, to in ((0, nxt), (1, prv), (2, far))
    ]
    rw_y = [at_y(yi + 1 - 2 * (yi % 2)), at_y(3 - yi)]

    def rw_send(k):
        return remote(rw.at[k], rw_in.at[k + 2], rw_y[k - 1], "rw", rw_in)

    def rw_add(k, copy):
        with scope(f"rw{k}"):
            copy.wait_recv()
            rw[k + 1] = rw[k] + rw_in[k + 2]

    loads[("x", 2)].wait()
    pre_part(2, 0)
    gather(0)
    pre_send(2, 0)
    pre_chip(0, 1)
    back_chip(0, 1)
    pre_part(2, 1)
    gather(1)
    pre_send(2, 1)
    loads[("x", 1)].wait()
    for a in range(2):
        pre_part(1, a)
        pre_send(1, a)
    hidden_of(0, 0)
    scaled_of(0, 0)
    with scope("rwx"):
        for copy in rw_x:
            copy.wait_recv()
        rw[1] = rw[0] + rw_in[0] + rw_in[1] + rw_in[2]
    rw_copy = rw_send(1)
    gs_wait(0, 0)
    cot_out(0, 0)
    shift(0, 0)
    hidden_of(0, 1)
    pre_chip(1, 0)
    scaled_of(0, 1)
    gs_wait(0, 1)
    cot_out(0, 1)
    shift(0, 1)

    rw_add(1, rw_copy)
    rw_copy = rw_send(2)
    pre_chip(1, 1)
    pre_chip(2, 0)
    pre_chip(2, 1)
    forward(0)
    hidden_of(1, 0)

    shift_in(1, 0)
    back_part(1, 0)
    back_send(1, 0)
    hidden_of(1, 1)
    back_chip(1, 0)
    forward(1)
    rw_add(2, rw_copy)
    loads["lg"].wait()
    with scope("entering"):

        @pl.when(top)
        def _():
            sums = rw[3]
            means = sums[0:1, :] / jnp.maximum(sums[1:2, :], 1.0)
            position = lax.broadcasted_iota(jnp.int32, (ROWS, 128), 0)
            for n in range(2):
                begin = jnp.int32(0)
                weights = jnp.zeros((ROWS, 128), F32)
                for k in range(SEQS):
                    finish = begin + lengths[n, 0, k]
                    own = jnp.sum(
                        jnp.where(lane[0:1, :] == ids[n, 0, k], means, 0.0), axis=-1, keepdims=True
                    )
                    advantage = rewards[n, 0, k] - own
                    inside = jnp.logical_and(position >= begin, position < finish)
                    weights = weights + jnp.where(inside, advantage, 0.0)
                    begin = finish
                weight[n] = -weights

                def body(i, carry):
                    r = sixteen(i * 16)
                    values = weight[n, r, 0:1] * lg[n, r, :].astype(F32)
                    call[1, sixteen((n + 1) * ROWS + i * 16), :] = values.astype(BF16)
                    return carry

                lax.fori_loop(0, ROWS // 16, body, 0)

    hidden_of(2, 0)
    scaled_of(1, 0)
    shift_in(1, 1)
    back_part(1, 1)
    back_send(1, 1)
    gs_wait(1, 0)
    cot_out(1, 0)
    shift(1, 0)

    out0x, out0y = (Ring(0, gout, 0, True, *split) for split in OUT_SPLITS[0])
    out1a, out1b, out1y = (Ring(2, gout, 1, True, *split) for split in OUT_SPLITS[1])
    in0, in1 = (Ring(1 + 2 * v, gin, v, False, *IN_SPLIT[0]) for v in range(2))
    hidden_of(2, 1)
    back_chip(1, 1)
    grad(1, gs, gained, 0, 2)
    in0.h(0)
    in0.f(0)
    for t in range(STEPS):
        for a in range(2):
            hid_copy[t, a].wait_recv()
    scaled_of(1, 1)
    gs_wait(1, 1)
    cot_out(1, 1)
    shift(1, 1)
    grad(3, gs, gained, 1, 2)
    in1.h(0)

    shift_in(2, 0)
    back_part(2, 0)
    back_send(2, 0)
    in0.m(0)
    grad(0, hid, call, 0, 3)
    back_chip(2, 0)
    out0x.h(0)
    out0x.f(0)
    scaled_of(2, 0)
    gs_wait(2, 0)
    left_send(0)
    out0y.h(0)
    shift_in(2, 1)
    back_part(2, 1)
    back_send(2, 1)
    grad(2, hid, call, 1, 3)
    back_chip(2, 1)
    out1a.h(0)
    out1b.h(0)
    out0x.m(0)
    cot_out(2, 0)
    out0y.m(0)
    out0y.f(0)
    in1.m(0)
    in1.f(0)
    in_middle(in0)
    scaled_of(2, 1)
    gs_wait(2, 1)
    left_send(1)
    out1y.h(0)
    out1a.m(0)
    out1b.m(0)
    out1a.f(0)
    out1b.f(0)
    out0x.middle()
    out0y.middle()
    cot_out(2, 1)
    in0.m(1)
    out1y.m(0)
    out1y.f(0)
    in_middle(in1)
    out1a.middle()
    out1b.middle()
    out0x.end()
    in0.end()
    out0y.end()
    out1y.middle()
    in1.m(1)
    in1.end()
    out1y.end()
    out1a.end()
    out1b.end()

    with scope("ends"):
        for sem, whole in classes.values():
            pltpu.make_async_remote_copy(
                src_ref=whole, dst_ref=whole, send_sem=sem, recv_sem=recv_sem.at[0],
                device_id=partner, device_id_type=MESH,
            ).wait_send()

        for t in range(STEPS - 1):
            for a in range(2):
                shift_do(t, a, lambda copy: copy.wait_send())
    assert (recv_used[0], len(classes), len(loads)) == (N_RECV, N_SEND, 15), (recv_used[0], len(classes), len(loads))


def finish(gin, gout, leaving, gin_hbm, gout_hbm, leaving_hbm, sem):
    pairs = ((leaving, leaving_hbm), (gin, gin_hbm), (gout, gout_hbm))
    copies = [pltpu.make_async_copy(src, dst, sem.at[k]) for k, (src, dst) in enumerate(pairs)]
    for copy in copies:
        copy.start()
    for copy in copies:
        copy.wait()


def shards(saved, proj_in, proj_out, gain, arriving, logp, rewards, lengths, ids):
    sections = lax.axis_size("pipe")
    hbm = pl.BlockSpec(memory_space=pltpu.HBM)
    vmem = pl.BlockSpec(memory_space=pltpu.VMEM)
    V = pltpu.VMEM
    shapes = (
        jax.ShapeDtypeStruct((2, 32, DL), F32),
        jax.ShapeDtypeStruct((2, 32, DL), F32),
        jax.ShapeDtypeStruct((2, ROWS, DL), BF16),
    )
    results = pl.pallas_call(
        lambda *refs: kernel(sections, *refs),
        name="window",
        out_shape=shapes,
        in_specs=[hbm] * 9,
        out_specs=(vmem, vmem, vmem),
        scratch_shapes=[
            V((STEPS, 2, ROWS, DL), BF16),
            V((2, R, DL), BF16),
            V((2, R, DL), BF16),
            V((2, 1, DL), F32),
            V((2, ROWS, DL), BF16),
            V((2, STEPS * ROWS, DL), BF16),
            V((2, STEPS * ROWS, DL), BF16),
            V((2, STEPS * ROWS, R), BF16),
            V((2, STEPS * ROWS, R), BF16),
            V((STEPS, 2, ROWS, 128), F32),
            V((STEPS, 2, ROWS, R), BF16),
            V((STEPS, 2, ROWS, R), BF16),
            V((STEPS, 2, HALF, R), BF16),
            V((STEPS, 2, HALF, R), BF16),
            V((STEPS, 2, HALF, R), BF16),
            V((STEPS, 2, HALF, R), BF16),
            V((STEPS, 2, HALF, R), BF16),
            V((STEPS, 2, HALF, R), BF16),
            V((ROWS, 128), F32),
            V((STEPS, 2, 8, 128), F32),
            V((STEPS, 2, 8, 128), F32),
            V((STEPS, 2, 8, 128), F32),
            V((STEPS, 2, 8, 128), F32),
            V((STEPS, 2, HALF, 128), F32),
            V((STEPS, 2, HALF, R), F32),
            V((STEPS, 2, HALF, R), F32),
            V((STEPS - 1, 2, ROWS, DL), BF16),
            V((4, 8, 128), F32),
            V((5, 8, 128), F32),
            V((2, ROWS, 128), F32),
            pltpu.SMEM((2, 1, SEQS), F32),
            pltpu.SMEM((2, 1, SEQS), jnp.int32),
            pltpu.SMEM((2, 1, SEQS), jnp.int32),
            V((4, 4, 4, 32, DL), BF16),
            V((4, 2, 2, 32, DL), BF16),
            V((4, 2, 4, 32, DL), BF16),
            V((4, 4, 32, DL), BF16),
            V((4, 2, 16, DL), BF16),
            V((4, 3, 32, DL), BF16),
            V((2, 3 * ROWS, DL), BF16),
            V((2, 3 * ROWS, 128), BF16),
            pltpu.SemaphoreType.DMA((15,)),
            pltpu.SemaphoreType.DMA((N_SEND,)),
            pltpu.SemaphoreType.DMA((N_RECV,)),
            pltpu.SemaphoreType.DMA((4,)),
            pltpu.SemaphoreType.DMA((4,)),
        ],
        compiler_params=pltpu.CompilerParams(
            collective_id=0, has_side_effects=True, vmem_limit_bytes=40 * 2**20
        ),
    )(
        *(
            pltpu.with_memory_space_constraint(x, pltpu.HBM)
            for x in (
                saved[:, :, 0], proj_in[:, 0], proj_out[:, 0], gain, arriving[:, 0], logp,
                rewards, lengths, ids,
            )
        )
    )
    any_spec = pl.BlockSpec(memory_space=pl.ANY)
    results = pl.pallas_call(
        finish,
        name="finish",
        out_shape=shapes,
        in_specs=[vmem] * 3,
        out_specs=(any_spec,) * 3,
        scratch_shapes=[pltpu.SemaphoreType.DMA((3,))],
        compiler_params=pltpu.CompilerParams(vmem_limit_bytes=2**20),
    )(*results)
    return tuple(r[:, None] for r in results)


def solution(mesh):
    return jax.shard_map(
        shards,
        mesh=mesh,
        in_specs=(
            P(None, None, "pipe", "dp", "tensor"),
            P(None, "pipe", None, "tensor"),
            P(None, "pipe", None, "tensor"),
            P(None, "pipe", "tensor"),
            P(None, "pipe", "dp", "tensor"),
            P(None, "dp", "tensor"),
            P(None, "dp", None),
            P(None, "dp", None),
            P(None, "dp", None),
        ),
        out_specs=(
            P(None, "pipe", "dp", "tensor"),
            P(None, "pipe", "dp", "tensor"),
            P(None, "pipe", "dp", "tensor"),
        ),
        check_vma=False,
    )
```
